32 devices in a mesh: radial: 8 (over z, x), phi: 4 (over y, core).
Axes of the slice: x: 2, y: 2, z: 4, core: 2. Of those that a mesh axis runs over, the one named last changes fastest.
Arguments:
- conserved: float32 [8, 64, 64, 128], P(None, 'radial', 'phi'), may hold values from -2.5 to 7, as said below
- core_mass: float32 [1], replicated, may hold values from 0.2 to 1
Outputs:
- advanced: float32 [8, 64, 64, 128], P(None, 'radial', 'phi')
- enclosed_mass: float32 [64], P('radial')
The draws below stay inside these ranges and needn't reach their ends.
Inputs may be any that keep to these rules, and one draw needn't show every extreme that they name: conserved[0] (density) lies between 0.4 and 2.5; conserved[4] exceeds (conserved[1]^2 + conserved[2]^2 + conserved[3]^2)/(2 conserved[0]) by at least 0.6; the speeds |conserved[m]/conserved[0]| stay below 1; conserved[5..7] lie between 0 and conserved[0].
All inputs are finite; a program needn't handle non-finite values.
Results may differ from the reference program's by a relative error of at most 0.0003.
Values sent between devices are 32-bit elements; how exact they have to be, the bound alone decides.
A program may use at most 64 MiB of HBM per device.

```python
import math
import jax
import jax.numpy as jnp
from jax import lax

RD = 8
NT = 128
NR = 64
NP = 64


def draw_conserved(key, part):
    subkeys = jax.random.split(key, 12)
    shape = (NR, NP, NT)
    depth = (jnp.arange(NR, dtype=jnp.float32) + 0.5) / NR
    azimuth = (jnp.arange(NP, dtype=jnp.float32) + 0.5) * (2.0 * math.pi / NP)
    centres = jax.random.uniform(subkeys[6], (3,), jnp.float32, 0.0, 1.0)
    heights = jax.random.uniform(subkeys[7], (3,), jnp.float32, -0.13, 0.13)
    bumps = jnp.exp(-jnp.square((depth[:, None] - centres[None, :]) / 0.15))
    profile = jnp.exp(jnp.sum(bumps * heights[None, :], axis=1))
    turn = jax.random.uniform(subkeys[8], (), jnp.float32, 0.0, 2.0 * math.pi)
    twist = jax.random.uniform(subkeys[9], (), jnp.float32, -0.5 * math.pi, 0.5 * math.pi)
    phase = turn + twist * depth
    angular = 1.0 + 0.35 * jnp.cos(azimuth[None, :] - phase[:, None])
    smooth = (profile[:, None] * angular)[:, :, None]
    rough = jnp.exp(jax.random.uniform(subkeys[0], shape, jnp.float32, jnp.log(0.75), jnp.log(1.33)))
    density = jnp.clip(smooth * rough, 0.4, 2.5)
    speeds = [jnp.clip(0.3 * jax.random.normal(subkeys[1 + which], shape, jnp.float32), -0.99, 0.99) for which in range(3)]
    pressure = jax.random.uniform(subkeys[4], shape, jnp.float32, 0.3, 0.9)
    kinetic = 0.5 * density * (speeds[0] * speeds[0] + speeds[1] * speeds[1] + speeds[2] * speeds[2])
    energy = pressure / (4.0 / 3.0 - 1.0) + kinetic
    tracers = jax.random.uniform(subkeys[5], (3,) + shape, jnp.float32, 0.0, 1.0) * density[None]
    momenta = jnp.stack([density * speeds[0], density * speeds[1], density * speeds[2]])
    return jnp.concatenate([density[None], momenta, energy[None], tracers], axis=0)


def setup_inputs(seed: int = 0) -> dict:
    streams_of = jax.random.split(jax.random.key(seed), 3)
    conserved = draw_conserved(jax.random.fold_in(streams_of[2], 71), 0)
    core_mass = jnp.clip(jnp.exp(jax.random.uniform(streams_of[1], (1,), jnp.float32, math.log(0.2), math.log(1.0))), 0.2, 1.0)
    return {"conserved": conserved, "core_mass": core_mass}


ADIABATIC = 4.0 / 3.0
INNER_RADIUS = 1.0
OUTER_RADIUS = 2.0
COURANT = 0.4
GRAVITY_KICK = 0.004
MINIMUM_DENSITY = 0.05
PRESSURE_FLOOR = 0.01

def step_sizes(radial_total, phi_total, theta_total):
    theta_step = math.pi / theta_total
    phi_step = 2.0 * math.pi / phi_total
    polar_width = INNER_RADIUS * math.sin(0.5 * theta_step) * phi_step
    radial_step = min(2.0 * polar_width, (OUTER_RADIUS - INNER_RADIUS) / radial_total)
    timestep = COURANT * min(radial_step, polar_width)
    return (radial_step, theta_step, phi_step, timestep)

def thermo(values):
    density = jnp.maximum(values[0], MINIMUM_DENSITY)
    kinetic = 0.5 * (values[1] * values[1] + values[2] * values[2] + values[3] * values[3]) / density
    pressure = jnp.maximum((ADIABATIC - 1.0) * (values[4] - kinetic), PRESSURE_FLOOR * density)
    return (density, pressure)

def physical(values, component):
    density, pressure = thermo(values)
    normal = values[component] / density
    sound = jnp.sqrt(ADIABATIC * pressure / density)
    pieces = [values[which] * normal for which in range(values.shape[0])]
    pieces[component] = pieces[component] + pressure
    pieces[4] = pieces[4] + pressure * normal
    return (jnp.stack(pieces), jnp.abs(normal) + sound)

def face_flux(values, along_dim, component):
    interior = values.shape[along_dim] - 4
    neighbour_differences = lax.slice_in_dim(values, 1, interior + 4, axis=along_dim) - lax.slice_in_dim(values, 0, interior + 3, axis=along_dim)
    below_diff = lax.slice_in_dim(neighbour_differences, 0, interior + 2, axis=along_dim)
    above_diff = lax.slice_in_dim(neighbour_differences, 1, interior + 3, axis=along_dim)
    limited = 0.5 * (jnp.sign(below_diff) + jnp.sign(above_diff)) * jnp.minimum(jnp.abs(below_diff), jnp.abs(above_diff))
    left_state = lax.slice_in_dim(values, 1, interior + 2, axis=along_dim) + 0.5 * lax.slice_in_dim(limited, 0, interior + 1, axis=along_dim)
    right_state = lax.slice_in_dim(values, 2, interior + 3, axis=along_dim) - 0.5 * lax.slice_in_dim(limited, 1, interior + 2, axis=along_dim)
    left_flux, left_signal = physical(left_state, component)
    right_flux, right_signal = physical(right_state, component)
    signal = jnp.maximum(left_signal, right_signal)
    return 0.5 * (left_flux + right_flux) - 0.5 * signal * (right_state - left_state)

def hydro_rate(extended, cell_centers, enclosed, radial_step, theta_step, phi_step, strength):
    theta_cells = extended.shape[3]
    centre_cells = extended[:, 2:-2, 2:-2, :]
    polar_padded = jnp.pad(centre_cells, ((0, 0), (0, 0), (0, 0), (2, 2)), mode='edge')
    radial_flux = face_flux(extended[:, :, 2:-2, :], 1, 1)
    polar_flux = face_flux(polar_padded, 3, 2)
    azimuth_flux = face_flux(extended[:, 2:-2, :, :], 2, 3)
    angles = (jnp.arange(theta_cells, dtype=jnp.float32) + 0.5) * theta_step
    sine_center = jnp.sin(angles)
    cosine = jnp.cos(angles)
    face_sine = jnp.sin(jnp.arange(theta_cells + 1, dtype=jnp.float32) * theta_step)
    radius = cell_centers[:, None, None]
    face_radius = jnp.concatenate([cell_centers - 0.5 * radial_step, cell_centers[-1:] + 0.5 * radial_step])[:, None, None]
    radial_area = face_radius * face_radius * radial_flux
    divergence = (radial_area[:, 1:] - radial_area[:, :-1]) / (radius * radius * radial_step)
    polar_area = face_sine * polar_flux
    divergence = divergence + (polar_area[..., 1:] - polar_area[..., :-1]) / (radius * sine_center * theta_step)
    divergence = divergence + (azimuth_flux[:, :, 1:] - azimuth_flux[:, :, :-1]) / (radius * sine_center * phi_step)
    density, pressure = thermo(centre_cells)
    radial_speed = centre_cells[1] / density
    polar_speed = centre_cells[2] / density
    azimuth_speed = centre_cells[3] / density
    cotangent = cosine / sine_center
    gravity_pull = strength * enclosed[:, None, None] / (radius * radius)
    source_radial = (2.0 * pressure + density * (polar_speed * polar_speed + azimuth_speed * azimuth_speed)) / radius - density * gravity_pull
    source_polar = (pressure * cotangent + density * azimuth_speed * azimuth_speed * cotangent - density * radial_speed * polar_speed) / radius
    source_azimuth = -density * azimuth_speed * (radial_speed + polar_speed * cotangent) / radius
    source_energy = -centre_cells[1] * gravity_pull
    nothing = jnp.zeros_like(pressure)
    source = jnp.stack([nothing, source_radial, source_polar, source_azimuth, source_energy, nothing, nothing, nothing])
    return source - divergence

def reference(conserved, core_mass):
    radial_total = conserved.shape[1]
    phi_total = conserved.shape[2]
    theta_total = conserved.shape[3]
    radial_step, theta_step, phi_step, timestep = step_sizes(radial_total, phi_total, theta_total)
    strength = GRAVITY_KICK / timestep
    cell_centers = INNER_RADIUS + (jnp.arange(radial_total, dtype=jnp.float32) + 0.5) * radial_step
    sine_center = jnp.sin((jnp.arange(theta_total, dtype=jnp.float32) + 0.5) * theta_step)
    shells = jnp.dot(lax.optimization_barrier(jnp.sum(conserved[0], axis=1)), sine_center, precision=lax.Precision.HIGHEST)
    shells = shells * cell_centers * cell_centers * (radial_step * theta_step * phi_step)
    enclosed = core_mass[0] + jnp.cumsum(shells) - 0.5 * shells
    blocks = radial_total // RD

    def full_rate(values):
        padded = jnp.pad(values, ((0, 0), (2, 2), (0, 0), (0, 0)), mode='edge')
        padded = jnp.pad(padded, ((0, 0), (0, 0), (2, 2), (0, 0)), mode='wrap')

        def one_block(block_index):
            first_row = (block_index * RD).astype(jnp.int32)
            radial_segment = lax.dynamic_slice_in_dim(padded, first_row, RD + 4, 1)
            radius_part = lax.dynamic_slice_in_dim(cell_centers, first_row, RD, 0)
            mass_part = lax.dynamic_slice_in_dim(enclosed, first_row, RD, 0)
            return hydro_rate(radial_segment, radius_part, mass_part, radial_step, theta_step, phi_step, strength)
        stacked = lax.map(one_block, jnp.arange(blocks, dtype=jnp.int32))
        return jnp.transpose(stacked, (1, 0, 2, 3, 4)).reshape(values.shape)
    section_one = conserved + timestep * full_rate(conserved)
    section_two = section_one + timestep * full_rate(section_one)
    advanced = 0.5 * conserved + 0.5 * section_two
    return (advanced, enclosed)
```

```python
import functools
import math

import jax
import jax.numpy as jnp
import numpy as np
from jax import lax
from jax.experimental import pallas as pl
from jax.experimental.pallas import tpu as pltpu
from jax.sharding import PartitionSpec as P

ADIABATIC = 4.0 / 3.0
INNER_RADIUS = 1.0
OUTER_RADIUS = 2.0
COURANT = 0.4
GRAVITY_KICK = 0.004
MINIMUM_DENSITY = 0.05
PRESSURE_FLOOR = 0.01
MESH = pl.DeviceIdType.MESH
TILE = 8
PAD = 8


def step_sizes(radial_total, phi_total, theta_total):
    theta_step = math.pi / theta_total
    phi_step = 2.0 * math.pi / phi_total
    polar_width = INNER_RADIUS * math.sin(0.5 * theta_step) * phi_step
    radial_step = min(2.0 * polar_width, (OUTER_RADIUS - INNER_RADIUS) / radial_total)
    timestep = COURANT * min(radial_step, polar_width)
    return (radial_step, theta_step, phi_step, timestep)


def angle_tables(theta_cells, theta_step):
    step = np.float32(theta_step)
    centre = (np.arange(theta_cells, dtype=np.float32) + np.float32(0.5)) * step
    face = np.arange(theta_cells + 1, dtype=np.float32) * step
    sine = np.sin(centre.astype(np.float64))
    cosine = np.cos(centre.astype(np.float64))
    face_sine = np.sin(face.astype(np.float64))
    zero = np.zeros(theta_cells)
    rows = [sine, face_sine[:-1], face_sine[1:], cosine / sine, 1.0 / sine, zero, zero, zero]
    return np.stack(rows).astype(np.float32)


def half_slope(below, above):
    return 0.5 * (
        jnp.maximum(jnp.minimum(below, above), 0.0) + jnp.minimum(jnp.maximum(below, above), 0.0)
    )


def thermo(q):
    density = jnp.maximum(q[0], MINIMUM_DENSITY)
    inverse = 1.0 / density
    kinetic = 0.5 * (q[1] * q[1] + q[2] * q[2] + q[3] * q[3]) * inverse
    pressure = jnp.maximum((ADIABATIC - 1.0) * (q[4] - kinetic), PRESSURE_FLOOR * density)
    return density, inverse, pressure


def physical(q, component):
    _, inverse, pressure = thermo(q)
    normal = q[component] * inverse
    squared = ADIABATIC * pressure * inverse
    return normal, pressure, jnp.abs(normal) + squared * lax.rsqrt(squared)


def flux(left, right, component):
    left_v, left_p, left_a = physical(left, component)
    right_v, right_p, right_a = physical(right, component)
    signal = jnp.maximum(left_a, right_a)
    left_w = 0.5 * (left_v + signal)
    right_w = 0.5 * (right_v - signal)
    out = [a * left_w + b * right_w for a, b in zip(left, right)]
    out[component] = out[component] + 0.5 * (left_p + right_p)
    out[4] = out[4] + 0.5 * (left_p * left_v + right_p * right_v)
    return out


def two_faces(rows, component):
    lower_left, lower_right, upper_left, upper_right = [], [], [], []
    for a, b, c, d, e in zip(*rows):
        ab, bc, cd, de = b - a, c - b, d - c, e - d
        sb, sc, sd = half_slope(ab, bc), half_slope(bc, cd), half_slope(cd, de)
        lower_left.append(b + sb)
        lower_right.append(c - sc)
        upper_left.append(c + sc)
        upper_right.append(d - sd)
    return flux(lower_left, lower_right, component), flux(upper_left, upper_right, component)


def kernel(
    sizes,
    counts,
    core_ref,
    table_ref,
    input_ref,
    out_ref,
    mass_ref,
    first,
    second,
    edge,
    halo,
    phi_part,
    phi_got,
    slab_part,
    slab_got,
    pull,
    load_sem,
    radial_send,
    radial_recv,
    phi_send,
    phi_recv,
    part_send,
    part_recv,
    slab_send,
    slab_recv,
):
    radial_step, theta_step, phi_step, timestep = sizes
    slabs, wedges = counts
    variables, rows, cells, lanes = input_ref.shape
    tiles = cells // TILE
    strength = GRAVITY_KICK / timestep
    slab, wedge = lax.axis_index("radial"), lax.axis_index("phi")
    has_up, has_down = slab < slabs - 1, slab > 0

    load = pltpu.make_async_copy(
        input_ref, first.at[:, pl.ds(2, rows), pl.ds(PAD, cells), :], load_sem
    )
    load.start()

    def radial_peer(jump):
        return (lax.rem(slab + jump, slabs), wedge)

    def phi_peer(jump):
        return (slab, lax.rem(wedge + jump, wedges))

    barrier = pltpu.get_barrier_semaphore()
    peers = [radial_peer(j) for j in range(1, slabs)] + [phi_peer(j) for j in range(1, wedges)]
    for peer in peers:
        pl.semaphore_signal(barrier, inc=1, device_id=peer, device_id_type=MESH)
    pl.semaphore_wait(barrier, len(peers))
    load.wait()

    def remote(src, dst, send, recv, peer):
        return pltpu.make_async_remote_copy(
            src_ref=src, dst_ref=dst, send_sem=send, recv_sem=recv, device_id=peer,
            device_id_type=MESH,
        )

    def radial_copies(buffer, section, tile):
        where = pl.ds(PAD + TILE * tile, TILE)
        slot = (section * tiles + tile) * 2
        up = remote(
            buffer.at[:, pl.ds(rows, 2), where, :], buffer.at[:, pl.ds(0, 2), where, :],
            radial_send.at[slot], radial_recv.at[slot], radial_peer(1),
        )
        down = remote(
            buffer.at[:, pl.ds(2, 2), where, :], buffer.at[:, pl.ds(rows + 2, 2), where, :],
            radial_send.at[slot + 1], radial_recv.at[slot + 1], radial_peer(slabs - 1),
        )
        return up, down

    def radial_start(copies):
        up, down = copies

        @pl.when(has_up)
        def _():
            up.start()

        @pl.when(has_down)
        def _():
            down.start()

    def radial_sent(copies):
        up, down = copies

        @pl.when(has_up)
        def _():
            up.wait_send()

        @pl.when(has_down)
        def _():
            down.wait_send()

    def radial_land(copies, buffer, tile):
        up, down = copies
        where = pl.ds(PAD + TILE * tile, TILE)

        @pl.when(has_down)
        def _():
            up.wait_recv()

        @pl.when(jnp.logical_not(has_down))
        def _():
            value = buffer[:, 2, where, :]
            buffer[:, 0, where, :] = value
            buffer[:, 1, where, :] = value

        @pl.when(has_up)
        def _():
            down.wait_recv()

        @pl.when(jnp.logical_not(has_up))
        def _():
            value = buffer[:, rows + 1, where, :]
            buffer[:, rows + 2, where, :] = value
            buffer[:, rows + 3, where, :] = value

    def phi_copies(section):
        slot = section * 2
        return [
            remote(
                edge.at[slot + side], halo.at[slot + side], phi_send.at[slot + side],
                phi_recv.at[slot + side], phi_peer(jump),
            )
            for side, jump in ((0, wedges - 1), (1, 1))
        ]

    def phi_pack(buffer, section, side):
        start = PAD if side == 0 else PAD + cells - 2
        edge[section * 2 + side] = buffer[:, pl.ds(2, rows), pl.ds(start, 2), :]

    def phi_unpack(buffer, section, side):
        start = PAD + cells if side == 0 else PAD - 2
        buffer[:, pl.ds(2, rows), pl.ds(start, 2), :] = halo[section * 2 + side]

    shape = (TILE, lanes)
    lane = lax.broadcasted_iota(jnp.int32, (rows, lanes), 1)
    line = lax.broadcasted_iota(jnp.int32, (rows, lanes), 0)
    column = jnp.sum(first[0, pl.ds(2, rows), pl.ds(PAD, cells), :], axis=1)
    column = jnp.sum(column * table_ref[0:1, :], axis=1, keepdims=True)
    centres = INNER_RADIUS + (
        (slab * rows + line).astype(jnp.float32) + 0.5
    ) * radial_step
    column = column * centres * centres * (radial_step * theta_step * phi_step)
    phi_part[...] = jnp.sum(jnp.where(lane == line, column, 0.0), axis=0, keepdims=True)
    part_copies = [
        remote(phi_part, phi_got.at[j], part_send.at[j], part_recv.at[j], phi_peer(j))
        for j in range(1, wedges)
    ]
    for copy in part_copies:
        copy.start()
    first_radial = [radial_copies(first, 0, t) for t in range(tiles)]
    second_radial = [radial_copies(second, 1, t) for t in range(tiles)]
    radial_start(first_radial[0])
    phi_pack(first, 0, 0)
    phi_pack(first, 0, 1)
    first_phi, second_phi = phi_copies(0), phi_copies(1)
    for copy in first_phi:
        copy.start()

    total = phi_part[...]
    for j, copy in enumerate(part_copies, 1):
        copy.wait_recv()
        total = total + phi_got[j]
    slab_part[...] = total
    slab_copies = [
        remote(slab_part, slab_got.at[j], slab_send.at[j], slab_recv.at[j], radial_peer(j))
        for j in range(1, slabs)
    ]
    for copy in slab_copies:
        copy.start()
    for t in range(1, tiles):
        radial_start(first_radial[t])

    lane_tile = lax.broadcasted_iota(jnp.int32, shape, 1)
    is_first, is_last = lane_tile == 0, lane_tile == lanes - 1

    def rate(buffer, r, tile):
        start = PAD + TILE * tile

        def at(row, offset):
            return [buffer[k, row + 2, pl.ds(start + offset, TILE), :] for k in range(variables)]

        def spread(value):
            return jnp.broadcast_to(value, shape)

        index = jnp.full(shape, slab * rows + r, jnp.int32).astype(jnp.float32)
        radius = INNER_RADIUS + (index + 0.5) * radial_step
        inner, outer = radius - 0.5 * radial_step, radius + 0.5 * radial_step
        inverse_r = 1.0 / radius
        centre = at(r, 0)
        lower, upper = two_faces([at(r + o, 0) if o else centre for o in range(-2, 3)], 1)
        scale = inverse_r * inverse_r * (1.0 / radial_step)
        area_in, area_out = inner * inner * scale, outer * outer * scale
        total = [area_in * a - area_out * b for a, b in zip(lower, upper)]
        lower, upper = two_faces([at(r, o) if o else centre for o in range(-2, 3)], 3)
        around = inverse_r * spread(table_ref[4:5, :])
        scale = around * (1.0 / phi_step)
        total = [t + (a - b) * scale for t, a, b in zip(total, lower, upper)]
        left, right = [], []
        for q in centre:
            after = jnp.where(is_last, q, pltpu.roll(q, lanes - 1, 1))
            above = after - q
            below = jnp.where(is_first, 0.0, pltpu.roll(above, 1, 1))
            slope = half_slope(below, above)
            left.append(q + slope)
            right.append(jnp.where(is_last, q, pltpu.roll(q - slope, lanes - 1, 1)))
        upper = flux(left, right, 2)
        scale = around * (1.0 / theta_step)
        low_sine, high_sine = spread(table_ref[1:2, :]), spread(table_ref[2:3, :])
        low_area, high_area = low_sine * scale, high_sine * scale
        total = [
            t + (low_area * pltpu.roll(f, 1, 1) - high_area * f) for t, f in zip(total, upper)
        ]
        density, inverse, pressure = thermo(centre)
        vr, vt, vp = (centre[m] * inverse for m in (1, 2, 3))
        cot = spread(table_ref[3:4, :])
        total[1] = total[1] + (2.0 * pressure + density * (vt * vt + vp * vp)) * inverse_r
        total[2] = total[2] + (
            (pressure + density * vp * vp) * cot - density * vr * vt
        ) * inverse_r
        total[3] = total[3] - density * vp * (vr + vt * cot) * inverse_r
        return centre, density, total, inverse_r

    def gravity_at(r):
        return jnp.broadcast_to(pull[pl.ds(r, 1), :], shape)

    def section_one(r, tile, with_gravity):
        centre, density, total, _ = rate(first, r, tile)
        if with_gravity:
            gravity = gravity_at(r)
            total[1] = total[1] - density * gravity
            total[4] = total[4] - centre[1] * gravity
        where = pl.ds(PAD + TILE * tile, TILE)
        for k in range(variables):
            second[k, r + 2, where, :] = centre[k] + timestep * total[k]

    def late_gravity(r, tile):
        where = pl.ds(PAD + TILE * tile, TILE)
        gravity = timestep * gravity_at(r)
        density = jnp.maximum(first[0, r + 2, where, :], MINIMUM_DENSITY)
        second[1, r + 2, where, :] = second[1, r + 2, where, :] - density * gravity
        second[4, r + 2, where, :] = (
            second[4, r + 2, where, :] - first[1, r + 2, where, :] * gravity
        )

    def section_two(r, tile):
        centre, density, total, _ = rate(second, r, tile)
        gravity = gravity_at(r)
        total[1] = total[1] - density * gravity
        total[4] = total[4] - centre[1] * gravity
        where = pl.ds(PAD + TILE * tile, TILE)
        into = pl.ds(TILE * tile, TILE)
        for k in range(variables):
            begin = first[k, r + 2, where, :]
            out_ref[k, r, into, :] = 0.5 * begin + 0.5 * (centre[k] + timestep * total[k])

    def each_row(low, high, step):
        lax.fori_loop(low, high, lambda r, _: (step(r), 0)[1], 0)

    def each_edge(step):
        lax.fori_loop(
            0, 4, lambda i, _: (step(i + (i // 2) * (rows - 4)), 0)[1], 0
        )

    def all_tiles(step):
        def run(r):
            for t in range(tiles):
                step(r, t)

        return run

    for side, copy in enumerate(first_phi):
        copy.wait_recv()
        phi_unpack(first, 0, side)
    each_row(2, rows - 2, all_tiles(lambda r, t: section_one(r, t, False)))

    before = jnp.zeros((1, lanes), jnp.float32)
    for j, copy in enumerate(slab_copies, 1):
        copy.wait_recv()
        before = before + jnp.where(slab >= j, slab_got[j], 0.0)
    before = jnp.sum(before, axis=1, keepdims=True)
    weight = jnp.where(lane < line, 1.0, jnp.where(lane == line, 0.5, 0.0))
    within = jnp.sum(weight * slab_part[...], axis=1, keepdims=True)
    enclosed = core_ref[0] + before + within + jnp.zeros((rows, lanes), jnp.float32)
    mass_ref[...] = jnp.sum(jnp.where(lane == line, enclosed, 0.0), axis=0, keepdims=True)[:, :rows]
    pull[...] = strength * enclosed / (centres * centres)
    each_row(2, rows - 2, all_tiles(late_gravity))

    for t in range(tiles):
        radial_land(first_radial[t], first, t)
        each_edge(lambda r: section_one(r, t, True))
        radial_start(second_radial[t])
        if t == 0:
            phi_pack(second, 1, 0)
            second_phi[0].start()
        if t == tiles - 1:
            phi_pack(second, 1, 1)
            second_phi[1].start()
    for side, copy in enumerate(second_phi):
        copy.wait_recv()
        phi_unpack(second, 1, side)
    each_row(2, rows - 2, all_tiles(section_two))
    for t in range(tiles):
        radial_land(second_radial[t], second, t)
        each_edge(lambda r: section_two(r, t))

    for copy in part_copies + slab_copies + first_phi + second_phi:
        copy.wait_send()
    for copies in first_radial + second_radial:
        radial_sent(copies)


def body(conserved, core_mass):
    variables, rows, cells, lanes = conserved.shape
    slabs, wedges = lax.axis_size("radial"), lax.axis_size("phi")
    sizes = step_sizes(rows * slabs, cells * wedges, lanes)
    table = jnp.asarray(angle_tables(lanes, sizes[1]))
    tiles = cells // TILE
    padded = (variables, rows + 4, cells + 2 * PAD, lanes)
    vmem = pl.BlockSpec(memory_space=pltpu.VMEM)
    dma = pltpu.SemaphoreType.DMA
    advanced, mass = pl.pallas_call(
        functools.partial(kernel, sizes, (slabs, wedges)),
        out_shape=(
            jax.ShapeDtypeStruct(conserved.shape, jnp.float32),
            jax.ShapeDtypeStruct((1, rows), jnp.float32),
        ),
        in_specs=[
            pl.BlockSpec(memory_space=pltpu.SMEM), vmem, pl.BlockSpec(memory_space=pl.ANY),
        ],
        out_specs=(vmem, vmem),
        scratch_shapes=[
            pltpu.VMEM(padded, jnp.float32),
            pltpu.VMEM(padded, jnp.float32),
            pltpu.VMEM((4, variables, rows, 2, lanes), jnp.float32),
            pltpu.VMEM((4, variables, rows, 2, lanes), jnp.float32),
            pltpu.VMEM((1, lanes), jnp.float32),
            pltpu.VMEM((wedges, 1, lanes), jnp.float32),
            pltpu.VMEM((1, lanes), jnp.float32),
            pltpu.VMEM((slabs, 1, lanes), jnp.float32),
            pltpu.VMEM((rows, lanes), jnp.float32),
            dma,
            dma((4 * tiles,)),
            dma((4 * tiles,)),
            dma((4,)),
            dma((4,)),
            dma((wedges,)),
            dma((wedges,)),
            dma((slabs,)),
            dma((slabs,)),
        ],
        compiler_params=pltpu.CompilerParams(collective_id=0, has_side_effects=True),
    )(core_mass, table, conserved)
    return advanced, mass.reshape(rows)


def solution(mesh):
    in_specs = (P(None, "radial", "phi", None), P())
    out_specs = (P(None, "radial", "phi", None), P("radial"))
    return jax.shard_map(body, mesh=mesh, in_specs=in_specs, out_specs=out_specs, check_vma=False)
```

```python
import functools
import math

import jax
import jax.numpy as jnp
import numpy as np
from jax import lax
from jax.experimental import pallas as pl
from jax.experimental.pallas import tpu as pltpu
from jax.sharding import PartitionSpec as P

ADIABATIC = 4.0 / 3.0
INNER_RADIUS = 1.0
OUTER_RADIUS = 2.0
COURANT = 0.4
GRAVITY_KICK = 0.004
MINIMUM_DENSITY = 0.05
PRESSURE_FLOOR = 0.01
MESH = pl.DeviceIdType.MESH
TILE = 8
PAD = 8


def step_sizes(radial_total, phi_total, theta_total):
    theta_step = math.pi / theta_total
    phi_step = 2.0 * math.pi / phi_total
    polar_width = INNER_RADIUS * math.sin(0.5 * theta_step) * phi_step
    radial_step = min(2.0 * polar_width, (OUTER_RADIUS - INNER_RADIUS) / radial_total)
    timestep = COURANT * min(radial_step, polar_width)
    return (radial_step, theta_step, phi_step, timestep)


def angle_tables(theta_cells, theta_step):
    step = np.float32(theta_step)
    centre = (np.arange(theta_cells, dtype=np.float32) + np.float32(0.5)) * step
    face = np.arange(theta_cells + 1, dtype=np.float32) * step
    sine = np.sin(centre.astype(np.float64))
    cosine = np.cos(centre.astype(np.float64))
    face_sine = np.sin(face.astype(np.float64))
    zero = np.zeros(theta_cells)
    rows = [sine, face_sine[:-1], face_sine[1:], cosine / sine, 1.0 / sine, zero, zero, zero]
    return np.stack(rows).astype(np.float32)


def half_slope(below, above):
    return 0.5 * (
        jnp.maximum(jnp.minimum(below, above), 0.0) + jnp.minimum(jnp.maximum(below, above), 0.0)
    )


def thermo(q):
    density = jnp.maximum(q[0], MINIMUM_DENSITY)
    inverse = 1.0 / density
    kinetic = 0.5 * (q[1] * q[1] + q[2] * q[2] + q[3] * q[3]) * inverse
    pressure = jnp.maximum((ADIABATIC - 1.0) * (q[4] - kinetic), PRESSURE_FLOOR * density)
    return density, inverse, pressure


def physical(q, component):
    _, inverse, pressure = thermo(q)
    normal = q[component] * inverse
    squared = ADIABATIC * pressure * inverse
    return normal, pressure, jnp.abs(normal) + squared * lax.rsqrt(squared)


def flux(left, right, component):
    left_v, left_p, left_a = physical(left, component)
    right_v, right_p, right_a = physical(right, component)
    signal = jnp.maximum(left_a, right_a)
    left_w = 0.5 * (left_v + signal)
    right_w = 0.5 * (right_v - signal)
    out = [a * left_w + b * right_w for a, b in zip(left, right)]
    out[component] = out[component] + 0.5 * (left_p + right_p)
    out[4] = out[4] + 0.5 * (left_p * left_v + right_p * right_v)
    return out


def two_faces(rows, component):
    lower_left, lower_right, upper_left, upper_right = [], [], [], []
    for a, b, c, d, e in zip(*rows):
        ab, bc, cd, de = b - a, c - b, d - c, e - d
        sb, sc, sd = half_slope(ab, bc), half_slope(bc, cd), half_slope(cd, de)
        lower_left.append(b + sb)
        lower_right.append(c - sc)
        upper_left.append(c + sc)
        upper_right.append(d - sd)
    return flux(lower_left, lower_right, component), flux(upper_left, upper_right, component)


def kernel(
    sizes,
    counts,
    core_ref,
    table_ref,
    input_ref,
    out_ref,
    mass_ref,
    first,
    second,
    edge,
    halo,
    phi_part,
    phi_got,
    slab_part,
    slab_got,
    pull,
    load_sem,
    radial_send,
    radial_recv,
    phi_send,
    phi_recv,
    part_send,
    part_recv,
    slab_send,
    slab_recv,
):
    radial_step, theta_step, phi_step, timestep = sizes
    slabs, wedges = counts
    variables, rows, cells, lanes = input_ref.shape
    tiles = cells // TILE
    strength = GRAVITY_KICK / timestep
    slab, wedge = lax.axis_index("radial"), lax.axis_index("phi")
    has_up, has_down = slab < slabs - 1, slab > 0

    load = pltpu.make_async_copy(
        input_ref, first.at[:, pl.ds(2, rows), pl.ds(PAD, cells), :], load_sem
    )
    load.start()

    def radial_peer(jump):
        return (lax.rem(slab + jump, slabs), wedge)

    def phi_peer(jump):
        return (slab, lax.rem(wedge + jump, wedges))

    barrier = pltpu.get_barrier_semaphore()
    peers = [radial_peer(j) for j in range(1, slabs)] + [phi_peer(j) for j in range(1, wedges)]
    for peer in peers:
        pl.semaphore_signal(barrier, inc=1, device_id=peer, device_id_type=MESH)
    pl.semaphore_wait(barrier, len(peers))
    load.wait()

    def remote(src, dst, send, recv, peer):
        return pltpu.make_async_remote_copy(
            src_ref=src, dst_ref=dst, send_sem=send, recv_sem=recv, device_id=peer,
            device_id_type=MESH,
        )

    def radial_copies(buffer, section, tile):
        where = pl.ds(PAD + TILE * tile, TILE)
        slot = (section * tiles + tile) * 2
        up = remote(
            buffer.at[:, pl.ds(rows, 2), where, :], buffer.at[:, pl.ds(0, 2), where, :],
            radial_send.at[slot], radial_recv.at[slot], radial_peer(1),
        )
        down = remote(
            buffer.at[:, pl.ds(2, 2), where, :], buffer.at[:, pl.ds(rows + 2, 2), where, :],
            radial_send.at[slot + 1], radial_recv.at[slot + 1], radial_peer(slabs - 1),
        )
        return up, down

    def radial_start(copies):
        up, down = copies

        @pl.when(has_up)
        def _():
            up.start()

        @pl.when(has_down)
        def _():
            down.start()

    def radial_sent(copies):
        up, down = copies

        @pl.when(has_up)
        def _():
            up.wait_send()

        @pl.when(has_down)
        def _():
            down.wait_send()

    def radial_land(copies, buffer, tile):
        up, down = copies
        where = pl.ds(PAD + TILE * tile, TILE)

        @pl.when(has_down)
        def _():
            up.wait_recv()

        @pl.when(jnp.logical_not(has_down))
        def _():
            value = buffer[:, 2, where, :]
            buffer[:, 0, where, :] = value
            buffer[:, 1, where, :] = value

        @pl.when(has_up)
        def _():
            down.wait_recv()

        @pl.when(jnp.logical_not(has_up))
        def _():
            value = buffer[:, rows + 1, where, :]
            buffer[:, rows + 2, where, :] = value
            buffer[:, rows + 3, where, :] = value

    def phi_copies(section):
        slot = section * 2
        return [
            remote(
                edge.at[slot + side], halo.at[slot + side], phi_send.at[slot + side],
                phi_recv.at[slot + side], phi_peer(jump),
            )
            for side, jump in ((0, wedges - 1), (1, 1))
        ]

    def phi_pack(buffer, section, side):
        start = PAD if side == 0 else PAD + cells - 2
        edge[section * 2 + side] = buffer[:, pl.ds(2, rows), pl.ds(start, 2), :]

    def phi_unpack(buffer, section, side):
        start = PAD + cells if side == 0 else PAD - 2
        buffer[:, pl.ds(2, rows), pl.ds(start, 2), :] = halo[section * 2 + side]

    shape = (TILE, lanes)
    lane = lax.broadcasted_iota(jnp.int32, (rows, lanes), 1)
    line = lax.broadcasted_iota(jnp.int32, (rows, lanes), 0)
    column = jnp.sum(first[0, pl.ds(2, rows), pl.ds(PAD, cells), :], axis=1)
    column = jnp.sum(column * table_ref[0:1, :], axis=1, keepdims=True)
    centres = INNER_RADIUS + (
        (slab * rows + line).astype(jnp.float32) + 0.5
    ) * radial_step
    column = column * centres * centres * (radial_step * theta_step * phi_step)
    phi_part[...] = jnp.sum(jnp.where(lane == line, column, 0.0), axis=0, keepdims=True)
    part_copies = [
        remote(phi_part, phi_got.at[j], part_send.at[j], part_recv.at[j], phi_peer(j))
        for j in range(1, wedges)
    ]
    for copy in part_copies:
        copy.start()
    first_radial = [radial_copies(first, 0, t) for t in range(tiles)]
    second_radial = [radial_copies(second, 1, t) for t in range(tiles)]
    radial_start(first_radial[0])
    phi_pack(first, 0, 0)
    phi_pack(first, 0, 1)
    first_phi, second_phi = phi_copies(0), phi_copies(1)
    for copy in first_phi:
        copy.start()

    total = phi_part[...]
    for j, copy in enumerate(part_copies, 1):
        copy.wait_recv()
        total = total + phi_got[j]
    slab_part[...] = total
    slab_copies = [
        remote(slab_part, slab_got.at[j], slab_send.at[j], slab_recv.at[j], radial_peer(j))
        for j in range(1, slabs)
    ]
    for copy in slab_copies:
        copy.start()
    for t in range(1, tiles):
        radial_start(first_radial[t])

    lane_tile = lax.broadcasted_iota(jnp.int32, shape, 1)
    is_first, is_last = lane_tile == 0, lane_tile == lanes - 1

    def rate(buffer, r, tile):
        start = PAD + TILE * tile

        def at(row, offset):
            return [buffer[k, row + 2, pl.ds(start + offset, TILE), :] for k in range(variables)]

        def spread(value):
            return jnp.broadcast_to(value, shape)

        index = jnp.full(shape, slab * rows + r, jnp.int32).astype(jnp.float32)
        radius = INNER_RADIUS + (index + 0.5) * radial_step
        inner, outer = radius - 0.5 * radial_step, radius + 0.5 * radial_step
        inverse_r = 1.0 / radius
        centre = at(r, 0)
        lower, upper = two_faces([at(r + o, 0) if o else centre for o in range(-2, 3)], 1)
        scale = inverse_r * inverse_r * (1.0 / radial_step)
        area_in, area_out = inner * inner * scale, outer * outer * scale
        total = [area_in * a - area_out * b for a, b in zip(lower, upper)]
        lower, upper = two_faces([at(r, o) if o else centre for o in range(-2, 3)], 3)
        around = inverse_r * spread(table_ref[4:5, :])
        scale = around * (1.0 / phi_step)
        total = [t + (a - b) * scale for t, a, b in zip(total, lower, upper)]
        left, right = [], []
        for q in centre:
            after = jnp.where(is_last, q, pltpu.roll(q, lanes - 1, 1))
            above = after - q
            below = jnp.where(is_first, 0.0, pltpu.roll(above, 1, 1))
            slope = half_slope(below, above)
            left.append(q + slope)
            right.append(jnp.where(is_last, q, pltpu.roll(q - slope, lanes - 1, 1)))
        upper = flux(left, right, 2)
        scale = around * (1.0 / theta_step)
        low_sine, high_sine = spread(table_ref[1:2, :]), spread(table_ref[2:3, :])
        low_area, high_area = low_sine * scale, high_sine * scale
        total = [
            t + (low_area * pltpu.roll(f, 1, 1) - high_area * f) for t, f in zip(total, upper)
        ]
        density, inverse, pressure = thermo(centre)
        vr, vt, vp = (centre[m] * inverse for m in (1, 2, 3))
        cot = spread(table_ref[3:4, :])
        total[1] = total[1] + (2.0 * pressure + density * (vt * vt + vp * vp)) * inverse_r
        total[2] = total[2] + (
            (pressure + density * vp * vp) * cot - density * vr * vt
        ) * inverse_r
        total[3] = total[3] - density * vp * (vr + vt * cot) * inverse_r
        return centre, density, total, inverse_r

    def gravity_at(r):
        return jnp.broadcast_to(pull[pl.ds(r, 1), :], shape)

    def section_one(r, tile, with_gravity):
        centre, density, total, _ = rate(first, r, tile)
        if with_gravity:
            gravity = gravity_at(r)
            total[1] = total[1] - density * gravity
            total[4] = total[4] - centre[1] * gravity
        where = pl.ds(PAD + TILE * tile, TILE)
        for k in range(variables):
            second[k, r + 2, where, :] = centre[k] + timestep * total[k]

    def late_gravity(r, tile):
        where = pl.ds(PAD + TILE * tile, TILE)
        gravity = timestep * gravity_at(r)
        density = jnp.maximum(first[0, r + 2, where, :], MINIMUM_DENSITY)
        second[1, r + 2, where, :] = second[1, r + 2, where, :] - density * gravity
        second[4, r + 2, where, :] = (
            second[4, r + 2, where, :] - first[1, r + 2, where, :] * gravity
        )

    def section_two(r, tile):
        centre, density, total, _ = rate(second, r, tile)
        gravity = gravity_at(r)
        total[1] = total[1] - density * gravity
        total[4] = total[4] - centre[1] * gravity
        where = pl.ds(PAD + TILE * tile, TILE)
        into = pl.ds(TILE * tile, TILE)
        for k in range(variables):
            begin = first[k, r + 2, where, :]
            out_ref[k, r, into, :] = 0.5 * begin + 0.5 * (centre[k] + timestep * total[k])

    def each_row(low, high, step):
        lax.fori_loop(low, high, lambda r, _: (step(r), 0)[1], 0)

    def each_edge(step):
        lax.fori_loop(
            0, 4, lambda i, _: (step(i + (i // 2) * (rows - 4)), 0)[1], 0
        )

    def all_tiles(step):
        def run(r):
            for t in range(tiles):
                step(r, t)

        return run

    for side, copy in enumerate(first_phi):
        copy.wait_recv()
        phi_unpack(first, 0, side)
    each_row(2, rows - 2, all_tiles(lambda r, t: section_one(r, t, False)))

    before = jnp.zeros((1, lanes), jnp.float32)
    for j, copy in enumerate(slab_copies, 1):
        copy.wait_recv()
        before = before + jnp.where(slab >= j, slab_got[j], 0.0)
    before = jnp.sum(before, axis=1, keepdims=True)
    weight = jnp.where(lane < line, 1.0, jnp.where(lane == line, 0.5, 0.0))
    within = jnp.sum(weight * slab_part[...], axis=1, keepdims=True)
    enclosed = core_ref[0] + before + within + jnp.zeros((rows, lanes), jnp.float32)
    mass_ref[...] = jnp.sum(jnp.where(lane == line, enclosed, 0.0), axis=0, keepdims=True)[:, :rows]
    pull[...] = strength * enclosed / (centres * centres)
    each_row(2, rows - 2, all_tiles(late_gravity))

    for t in range(tiles):
        radial_land(first_radial[t], first, t)
        each_edge(lambda r: section_one(r, t, True))
        radial_start(second_radial[t])
        if t == 0:
            phi_pack(second, 1, 0)
            second_phi[0].start()
        if t == tiles - 1:
            phi_pack(second, 1, 1)
            second_phi[1].start()
    for side, copy in enumerate(second_phi):
        copy.wait_recv()
        phi_unpack(second, 1, side)
    each_row(2, rows - 2, all_tiles(section_two))
    for t in range(tiles):
        radial_land(second_radial[t], second, t)
        each_edge(lambda r: section_two(r, t))

    for copy in part_copies + slab_copies + first_phi + second_phi:
        copy.wait_send()
    for copies in first_radial + second_radial:
        radial_sent(copies)


def body(conserved, core_mass):
    variables, rows, cells, lanes = conserved.shape
    slabs, wedges = lax.axis_size("radial"), lax.axis_size("phi")
    sizes = step_sizes(rows * slabs, cells * wedges, lanes)
    table = jnp.asarray(angle_tables(lanes, sizes[1]))
    tiles = cells // TILE
    padded = (variables, rows + 4, cells + 2 * PAD, lanes)
    vmem = pl.BlockSpec(memory_space=pltpu.VMEM)
    dma = pltpu.SemaphoreType.DMA
    advanced, mass = pl.pallas_call(
        functools.partial(kernel, sizes, (slabs, wedges)),
        out_shape=(
            pltpu.VMEM(conserved.shape, jnp.float32),
            pltpu.VMEM((1, rows), jnp.float32),
        ),
        in_specs=[
            pl.BlockSpec(memory_space=pltpu.SMEM), vmem, pl.BlockSpec(memory_space=pl.ANY),
        ],
        out_specs=(vmem, vmem),
        scratch_shapes=[
            pltpu.VMEM(padded, jnp.float32),
            pltpu.VMEM(padded, jnp.float32),
            pltpu.VMEM((4, variables, rows, 2, lanes), jnp.float32),
            pltpu.VMEM((4, variables, rows, 2, lanes), jnp.float32),
            pltpu.VMEM((1, lanes), jnp.float32),
            pltpu.VMEM((wedges, 1, lanes), jnp.float32),
            pltpu.VMEM((1, lanes), jnp.float32),
            pltpu.VMEM((slabs, 1, lanes), jnp.float32),
            pltpu.VMEM((rows, lanes), jnp.float32),
            dma,
            dma((4 * tiles,)),
            dma((4 * tiles,)),
            dma((4,)),
            dma((4,)),
            dma((wedges,)),
            dma((wedges,)),
            dma((slabs,)),
            dma((slabs,)),
        ],
        compiler_params=pltpu.CompilerParams(collective_id=0, has_side_effects=True),
    )(core_mass, table, conserved)
    return advanced, mass.reshape(rows)


def solution(mesh):
    in_specs = (P(None, "radial", "phi", None), P())
    out_specs = (P(None, "radial", "phi", None), P("radial"))
    return jax.shard_map(body, mesh=mesh, in_specs=in_specs, out_specs=out_specs, check_vma=False)
```

```python
import functools
import math

import jax
import jax.numpy as jnp
import numpy as np
from jax import lax
from jax.experimental import pallas as pl
from jax.experimental.pallas import tpu as pltpu
from jax.sharding import PartitionSpec as P

ADIABATIC = 4.0 / 3.0
INNER_RADIUS = 1.0
OUTER_RADIUS = 2.0
COURANT = 0.4
GRAVITY_KICK = 0.004
MINIMUM_DENSITY = 0.05
PRESSURE_FLOOR = 0.01
MESH = pl.DeviceIdType.MESH
TILE = 8
PAD = 8


def step_sizes(radial_total, phi_total, theta_total):
    theta_step = math.pi / theta_total
    phi_step = 2.0 * math.pi / phi_total
    polar_width = INNER_RADIUS * math.sin(0.5 * theta_step) * phi_step
    radial_step = min(2.0 * polar_width, (OUTER_RADIUS - INNER_RADIUS) / radial_total)
    timestep = COURANT * min(radial_step, polar_width)
    return (radial_step, theta_step, phi_step, timestep)


def angle_tables(theta_cells, theta_step):
    step = np.float32(theta_step)
    centre = (np.arange(theta_cells, dtype=np.float32) + np.float32(0.5)) * step
    face = np.arange(theta_cells + 1, dtype=np.float32) * step
    sine = np.sin(centre.astype(np.float64))
    cosine = np.cos(centre.astype(np.float64))
    face_sine = np.sin(face.astype(np.float64))
    zero = np.zeros(theta_cells)
    rows = [sine, face_sine[:-1], face_sine[1:], cosine / sine, 1.0 / sine, zero, zero, zero]
    return np.stack(rows).astype(np.float32)


def half_slope(below, above):
    return 0.5 * (
        jnp.maximum(jnp.minimum(below, above), 0.0) + jnp.minimum(jnp.maximum(below, above), 0.0)
    )


def thermo(q):
    density = jnp.maximum(q[0], MINIMUM_DENSITY)
    inverse = 1.0 / density
    kinetic = 0.5 * (q[1] * q[1] + q[2] * q[2] + q[3] * q[3]) * inverse
    pressure = jnp.maximum((ADIABATIC - 1.0) * (q[4] - kinetic), PRESSURE_FLOOR * density)
    return density, inverse, pressure


def physical(q, component):
    _, inverse, pressure = thermo(q)
    normal = q[component] * inverse
    squared = ADIABATIC * pressure * inverse
    return normal, pressure, jnp.abs(normal) + squared * lax.rsqrt(squared)


def flux(left, right, component):
    left_v, left_p, left_a = physical(left, component)
    right_v, right_p, right_a = physical(right, component)
    signal = jnp.maximum(left_a, right_a)
    left_w = 0.5 * (left_v + signal)
    right_w = 0.5 * (right_v - signal)
    out = [a * left_w + b * right_w for a, b in zip(left, right)]
    out[component] = out[component] + 0.5 * (left_p + right_p)
    out[4] = out[4] + 0.5 * (left_p * left_v + right_p * right_v)
    return out


def two_faces(rows, component):
    lower_left, lower_right, upper_left, upper_right = [], [], [], []
    for a, b, c, d, e in zip(*rows):
        ab, bc, cd, de = b - a, c - b, d - c, e - d
        sb, sc, sd = half_slope(ab, bc), half_slope(bc, cd), half_slope(cd, de)
        lower_left.append(b + sb)
        lower_right.append(c - sc)
        upper_left.append(c + sc)
        upper_right.append(d - sd)
    return flux(lower_left, lower_right, component), flux(upper_left, upper_right, component)


def kernel(
    sizes,
    counts,
    core_ref,
    table_ref,
    input_ref,
    out_ref,
    mass_ref,
    first,
    second,
    edge,
    halo,
    part,
    got,
    pull,
    table,
    core,
    load_sem,
    radial_send,
    radial_recv,
    phi_send,
    phi_recv,
    part_send,
    part_recv,
):
    radial_step, theta_step, phi_step, timestep = sizes
    slabs, wedges = counts
    variables, rows, cells, lanes = input_ref.shape
    tiles = cells // TILE
    strength = GRAVITY_KICK / timestep
    slab, wedge = lax.axis_index("radial"), lax.axis_index("phi")
    has_up, has_down = slab < slabs - 1, slab > 0

    load = pltpu.make_async_copy(
        input_ref, first.at[:, pl.ds(2, rows), pl.ds(PAD, cells), :], load_sem.at[0]
    )
    load.start()
    load_table = pltpu.make_async_copy(table_ref, table, load_sem.at[1])
    load_table.start()
    load_core = pltpu.make_async_copy(core_ref, core, load_sem.at[2])
    load_core.start()

    def radial_peer(jump):
        return (lax.rem(slab + jump, slabs), wedge)

    def phi_peer(jump):
        return (slab, lax.rem(wedge + jump, wedges))

    barrier = pltpu.get_barrier_semaphore()
    jumps = [(i, j) for i in range(slabs) for j in range(wedges) if i or j]

    def peer_at(jump):
        return (radial_peer(jump[0])[0], phi_peer(jump[1])[1])

    for jump in jumps:
        pl.semaphore_signal(barrier, inc=1, device_id=peer_at(jump), device_id_type=MESH)
    load.wait()
    load_table.wait()
    load_core.wait()

    def remote(src, dst, send, recv, peer):
        return pltpu.make_async_remote_copy(
            src_ref=src, dst_ref=dst, send_sem=send, recv_sem=recv, device_id=peer,
            device_id_type=MESH,
        )

    def radial_copies(buffer, section, tile):
        where = pl.ds(PAD + TILE * tile, TILE)
        slot = (section * tiles + tile) * 2
        up = remote(
            buffer.at[:, pl.ds(rows, 2), where, :], buffer.at[:, pl.ds(0, 2), where, :],
            radial_send.at[slot], radial_recv.at[slot], radial_peer(1),
        )
        down = remote(
            buffer.at[:, pl.ds(2, 2), where, :], buffer.at[:, pl.ds(rows + 2, 2), where, :],
            radial_send.at[slot + 1], radial_recv.at[slot + 1], radial_peer(slabs - 1),
        )
        return up, down

    def radial_start(copies):
        up, down = copies

        @pl.when(has_up)
        def _():
            up.start()

        @pl.when(has_down)
        def _():
            down.start()

    def radial_sent(copies):
        up, down = copies

        @pl.when(has_up)
        def _():
            up.wait_send()

        @pl.when(has_down)
        def _():
            down.wait_send()

    def radial_land(copies, buffer, tile):
        up, down = copies
        where = pl.ds(PAD + TILE * tile, TILE)

        @pl.when(has_down)
        def _():
            up.wait_recv()

        @pl.when(jnp.logical_not(has_down))
        def _():
            value = buffer[:, 2, where, :]
            buffer[:, 0, where, :] = value
            buffer[:, 1, where, :] = value

        @pl.when(has_up)
        def _():
            down.wait_recv()

        @pl.when(jnp.logical_not(has_up))
        def _():
            value = buffer[:, rows + 1, where, :]
            buffer[:, rows + 2, where, :] = value
            buffer[:, rows + 3, where, :] = value

    def phi_copies(section):
        slot = section * 2
        return [
            remote(
                edge.at[slot + side], halo.at[slot + side], phi_send.at[slot + side],
                phi_recv.at[slot + side], phi_peer(jump),
            )
            for side, jump in ((0, wedges - 1), (1, 1))
        ]

    def phi_pack(buffer, section, side):
        start = PAD if side == 0 else PAD + cells - 2
        edge[section * 2 + side] = buffer[:, pl.ds(2, rows), pl.ds(start, 2), :]

    def phi_unpack(buffer, section, side):
        start = PAD + cells if side == 0 else PAD - 2
        buffer[:, pl.ds(2, rows), pl.ds(start, 2), :] = halo[section * 2 + side]

    shape = (TILE, lanes)
    lane = lax.broadcasted_iota(jnp.int32, (rows, lanes), 1)
    line = lax.broadcasted_iota(jnp.int32, (rows, lanes), 0)
    column = jnp.sum(first[0, pl.ds(2, rows), pl.ds(PAD, cells), :], axis=1)
    column = jnp.sum(column * table[0:1, :], axis=1, keepdims=True)
    centres = INNER_RADIUS + (
        (slab * rows + line).astype(jnp.float32) + 0.5
    ) * radial_step
    column = column * centres * centres * (radial_step * theta_step * phi_step)
    part[...] = jnp.sum(jnp.where(lane == line, column, 0.0), axis=0, keepdims=True)
    got[0] = part[...]
    phi_pack(first, 0, 0)
    phi_pack(first, 0, 1)
    pl.semaphore_wait(barrier, len(jumps))

    part_copies = []
    for i, j in jumps:
        slot = i * wedges + j
        part_copies.append(
            remote(part, got.at[slot], part_send.at[slot], part_recv.at[slot], peer_at((i, j)))
        )
    first_radial = [radial_copies(first, 0, t) for t in range(tiles)]
    second_radial = [radial_copies(second, 1, t) for t in range(tiles)]
    first_phi, second_phi = phi_copies(0), phi_copies(1)
    for copy in first_phi + part_copies:
        copy.start()
    for t in range(tiles):
        radial_start(first_radial[t])

    lane_tile = lax.broadcasted_iota(jnp.int32, shape, 1)
    is_first, is_last = lane_tile == 0, lane_tile == lanes - 1

    def rate(buffer, r, tile):
        start = PAD + TILE * tile

        def at(row, offset):
            return [buffer[k, row + 2, pl.ds(start + offset, TILE), :] for k in range(variables)]

        def spread(value):
            return jnp.broadcast_to(value, shape)

        index = jnp.full(shape, slab * rows + r, jnp.int32).astype(jnp.float32)
        radius = INNER_RADIUS + (index + 0.5) * radial_step
        inner, outer = radius - 0.5 * radial_step, radius + 0.5 * radial_step
        inverse_r = 1.0 / radius
        centre = at(r, 0)
        lower, upper = two_faces([at(r + o, 0) if o else centre for o in range(-2, 3)], 1)
        scale = inverse_r * inverse_r * (1.0 / radial_step)
        area_in, area_out = inner * inner * scale, outer * outer * scale
        total = [area_in * a - area_out * b for a, b in zip(lower, upper)]
        lower, upper = two_faces([at(r, o) if o else centre for o in range(-2, 3)], 3)
        around = inverse_r * spread(table[4:5, :])
        scale = around * (1.0 / phi_step)
        total = [t + (a - b) * scale for t, a, b in zip(total, lower, upper)]
        left, right = [], []
        for q in centre:
            after = jnp.where(is_last, q, pltpu.roll(q, lanes - 1, 1))
            above = after - q
            below = jnp.where(is_first, 0.0, pltpu.roll(above, 1, 1))
            slope = half_slope(below, above)
            left.append(q + slope)
            right.append(jnp.where(is_last, q, pltpu.roll(q - slope, lanes - 1, 1)))
        upper = flux(left, right, 2)
        scale = around * (1.0 / theta_step)
        low_sine, high_sine = spread(table[1:2, :]), spread(table[2:3, :])
        low_area, high_area = low_sine * scale, high_sine * scale
        total = [
            t + (low_area * pltpu.roll(f, 1, 1) - high_area * f) for t, f in zip(total, upper)
        ]
        density, inverse, pressure = thermo(centre)
        vr, vt, vp = (centre[m] * inverse for m in (1, 2, 3))
        cot = spread(table[3:4, :])
        total[1] = total[1] + (2.0 * pressure + density * (vt * vt + vp * vp)) * inverse_r
        total[2] = total[2] + (
            (pressure + density * vp * vp) * cot - density * vr * vt
        ) * inverse_r
        total[3] = total[3] - density * vp * (vr + vt * cot) * inverse_r
        return centre, density, total, inverse_r

    def gravity_at(r):
        return jnp.broadcast_to(pull[pl.ds(r, 1), :], shape)

    def section_one(r, tile, with_gravity):
        centre, density, total, _ = rate(first, r, tile)
        if with_gravity:
            gravity = gravity_at(r)
            total[1] = total[1] - density * gravity
            total[4] = total[4] - centre[1] * gravity
        where = pl.ds(PAD + TILE * tile, TILE)
        for k in range(variables):
            second[k, r + 2, where, :] = centre[k] + timestep * total[k]

    def late_gravity(r, tile):
        where = pl.ds(PAD + TILE * tile, TILE)
        gravity = timestep * gravity_at(r)
        density = jnp.maximum(first[0, r + 2, where, :], MINIMUM_DENSITY)
        second[1, r + 2, where, :] = second[1, r + 2, where, :] - density * gravity
        second[4, r + 2, where, :] = (
            second[4, r + 2, where, :] - first[1, r + 2, where, :] * gravity
        )

    def section_two(r, tile):
        centre, density, total, _ = rate(second, r, tile)
        gravity = gravity_at(r)
        total[1] = total[1] - density * gravity
        total[4] = total[4] - centre[1] * gravity
        where = pl.ds(PAD + TILE * tile, TILE)
        into = pl.ds(TILE * tile, TILE)
        for k in range(variables):
            begin = first[k, r + 2, where, :]
            out_ref[k, r, into, :] = 0.5 * begin + 0.5 * (centre[k] + timestep * total[k])

    def each_row(low, high, step):
        lax.fori_loop(low, high, lambda r, _: (step(r), 0)[1], 0)

    def each_edge(step):
        lax.fori_loop(
            0, 4, lambda i, _: (step(i + (i // 2) * (rows - 4)), 0)[1], 0
        )

    def all_tiles(step):
        def run(r):
            for t in range(tiles):
                step(r, t)

        return run

    for side, copy in enumerate(first_phi):
        copy.wait_recv()
        phi_unpack(first, 0, side)
    each_row(2, rows - 2, all_tiles(lambda r, t: section_one(r, t, False)))

    for copy in part_copies:
        copy.wait_recv()

    def slab_shells(jump):
        shells = jnp.zeros((1, lanes), jnp.float32)
        for w in range(wedges):
            shells = shells + got[jump * wedges + lax.rem(wedge + wedges - w, wedges)]
        return shells

    before = jnp.zeros((1, lanes), jnp.float32)
    for j in range(slabs - 1, 0, -1):
        before = before + jnp.where(slab >= j, slab_shells(j), 0.0)
    before = jnp.sum(before, axis=1, keepdims=True)
    weight = jnp.where(lane < line, 1.0, jnp.where(lane == line, 0.5, 0.0))
    within = jnp.sum(weight * slab_shells(0), axis=1, keepdims=True)
    enclosed = core[0] + before + within + jnp.zeros((rows, lanes), jnp.float32)
    mass_ref[...] = jnp.sum(jnp.where(lane == line, enclosed, 0.0), axis=0, keepdims=True)[:, :rows]
    pull[...] = strength * enclosed / (centres * centres)
    each_row(2, rows - 2, all_tiles(late_gravity))

    for t in range(tiles):
        radial_land(first_radial[t], first, t)
        each_edge(lambda r: section_one(r, t, True))
        radial_start(second_radial[t])
        if t == 0:
            phi_pack(second, 1, 0)
            second_phi[0].start()
        if t == tiles - 1:
            phi_pack(second, 1, 1)
            second_phi[1].start()
    for side, copy in enumerate(second_phi):
        copy.wait_recv()
        phi_unpack(second, 1, side)
    each_row(2, rows - 2, all_tiles(section_two))
    for t in range(tiles):
        radial_land(second_radial[t], second, t)
        each_edge(lambda r: section_two(r, t))

    for copy in part_copies + first_phi + second_phi:
        copy.wait_send()
    for copies in first_radial + second_radial:
        radial_sent(copies)


def body(conserved, core_mass):
    variables, rows, cells, lanes = conserved.shape
    slabs, wedges = lax.axis_size("radial"), lax.axis_size("phi")
    sizes = step_sizes(rows * slabs, cells * wedges, lanes)
    table = jnp.asarray(angle_tables(lanes, sizes[1]))
    tiles = cells // TILE
    padded = (variables, rows + 4, cells + 2 * PAD, lanes)
    vmem = pl.BlockSpec(memory_space=pltpu.VMEM)
    dma = pltpu.SemaphoreType.DMA
    advanced, mass = pl.pallas_call(
        functools.partial(kernel, sizes, (slabs, wedges)),
        out_shape=(
            pltpu.VMEM(conserved.shape, jnp.float32),
            pltpu.VMEM((1, rows), jnp.float32),
        ),
        in_specs=[pl.BlockSpec(memory_space=pl.ANY)] * 3,
        out_specs=(vmem, vmem),
        scratch_shapes=[
            pltpu.VMEM(padded, jnp.float32),
            pltpu.VMEM(padded, jnp.float32),
            pltpu.VMEM((4, variables, rows, 2, lanes), jnp.float32),
            pltpu.VMEM((4, variables, rows, 2, lanes), jnp.float32),
            pltpu.VMEM((1, lanes), jnp.float32),
            pltpu.VMEM((slabs * wedges, 1, lanes), jnp.float32),
            pltpu.VMEM((rows, lanes), jnp.float32),
            pltpu.VMEM((TILE, lanes), jnp.float32),
            pltpu.SMEM((1,), jnp.float32),
            dma((3,)),
            dma((4 * tiles,)),
            dma((4 * tiles,)),
            dma((4,)),
            dma((4,)),
            dma((slabs * wedges,)),
            dma((slabs * wedges,)),
        ],
        compiler_params=pltpu.CompilerParams(collective_id=0, has_side_effects=True),
    )(core_mass, table, conserved)
    return advanced, mass.reshape(rows)


def solution(mesh):
    in_specs = (P(None, "radial", "phi", None), P())
    out_specs = (P(None, "radial", "phi", None), P("radial"))
    return jax.shard_map(body, mesh=mesh, in_specs=in_specs, out_specs=out_specs, check_vma=False)
```

```python
import functools
import math

import jax
import jax.numpy as jnp
import numpy as np
from jax import lax
from jax.experimental import pallas as pl
from jax.experimental.pallas import tpu as pltpu
from jax.sharding import PartitionSpec as P

ADIABATIC = 4.0 / 3.0
INNER_RADIUS = 1.0
OUTER_RADIUS = 2.0
COURANT = 0.4
GRAVITY_KICK = 0.004
MINIMUM_DENSITY = 0.05
PRESSURE_FLOOR = 0.01
MESH = pl.DeviceIdType.MESH
TILE = 8
PAD = 8


def step_sizes(radial_total, phi_total, theta_total):
    theta_step = math.pi / theta_total
    phi_step = 2.0 * math.pi / phi_total
    polar_width = INNER_RADIUS * math.sin(0.5 * theta_step) * phi_step
    radial_step = min(2.0 * polar_width, (OUTER_RADIUS - INNER_RADIUS) / radial_total)
    timestep = COURANT * min(radial_step, polar_width)
    return (radial_step, theta_step, phi_step, timestep)


def angle_tables(theta_cells, theta_step):
    step = np.float32(theta_step)
    centre = (np.arange(theta_cells, dtype=np.float32) + np.float32(0.5)) * step
    face = np.arange(theta_cells + 1, dtype=np.float32) * step
    sine = np.sin(centre.astype(np.float64))
    cosine = np.cos(centre.astype(np.float64))
    face_sine = np.sin(face.astype(np.float64))
    zero = np.zeros(theta_cells)
    rows = [sine, face_sine[:-1], face_sine[1:], cosine / sine, 1.0 / sine, zero, zero, zero]
    return np.stack(rows).astype(np.float32)


def half_slope(below, above):
    return 0.5 * (
        jnp.maximum(jnp.minimum(below, above), 0.0) + jnp.minimum(jnp.maximum(below, above), 0.0)
    )


def thermo(q):
    density = jnp.maximum(q[0], MINIMUM_DENSITY)
    inverse = 1.0 / density
    kinetic = 0.5 * (q[1] * q[1] + q[2] * q[2] + q[3] * q[3]) * inverse
    pressure = jnp.maximum((ADIABATIC - 1.0) * (q[4] - kinetic), PRESSURE_FLOOR * density)
    return density, inverse, pressure


def physical(q, component):
    _, inverse, pressure = thermo(q)
    normal = q[component] * inverse
    squared = ADIABATIC * pressure * inverse
    return normal, pressure, jnp.abs(normal) + squared * lax.rsqrt(squared)


def flux(left, right, component):
    left_v, left_p, left_a = physical(left, component)
    right_v, right_p, right_a = physical(right, component)
    signal = jnp.maximum(left_a, right_a)
    left_w = 0.5 * (left_v + signal)
    right_w = 0.5 * (right_v - signal)
    out = [a * left_w + b * right_w for a, b in zip(left, right)]
    out[component] = out[component] + 0.5 * (left_p + right_p)
    out[4] = out[4] + 0.5 * (left_p * left_v + right_p * right_v)
    return out


def two_faces(rows, component):
    lower_left, lower_right, upper_left, upper_right = [], [], [], []
    for a, b, c, d, e in zip(*rows):
        ab, bc, cd, de = b - a, c - b, d - c, e - d
        sb, sc, sd = half_slope(ab, bc), half_slope(bc, cd), half_slope(cd, de)
        lower_left.append(b + sb)
        lower_right.append(c - sc)
        upper_left.append(c + sc)
        upper_right.append(d - sd)
    return flux(lower_left, lower_right, component), flux(upper_left, upper_right, component)


def kernel(
    sizes,
    counts,
    core_ref,
    table_ref,
    input_ref,
    out_ref,
    mass_ref,
    first,
    second,
    edge,
    halo,
    part,
    got,
    pull,
    table,
    core,
    load_sem,
    radial_send,
    radial_recv,
    phi_send,
    phi_recv,
    part_send,
    part_recv,
):
    radial_step, theta_step, phi_step, timestep = sizes
    slabs, wedges = counts
    variables, rows, cells, lanes = input_ref.shape
    tiles = cells // TILE
    strength = GRAVITY_KICK / timestep
    slab, wedge = lax.axis_index("radial"), lax.axis_index("phi")
    has_up, has_down = slab < slabs - 1, slab > 0

    load = pltpu.make_async_copy(
        input_ref, first.at[:, pl.ds(2, rows), pl.ds(PAD, cells), :], load_sem.at[0]
    )
    load.start()
    load_table = pltpu.make_async_copy(table_ref, table, load_sem.at[1])
    load_table.start()
    load_core = pltpu.make_async_copy(core_ref, core, load_sem.at[2])
    load_core.start()

    def radial_peer(jump):
        return (lax.rem(slab + jump, slabs), wedge)

    def phi_peer(jump):
        return (slab, lax.rem(wedge + jump, wedges))

    barrier = pltpu.get_barrier_semaphore()
    jumps = [(i, j) for i in range(slabs) for j in range(wedges) if i or j]

    def peer_at(jump):
        return (radial_peer(jump[0])[0], phi_peer(jump[1])[1])

    for jump in jumps:
        pl.semaphore_signal(barrier, inc=1, device_id=peer_at(jump), device_id_type=MESH)
    load.wait()
    load_table.wait()
    load_core.wait()

    def remote(src, dst, send, recv, peer):
        return pltpu.make_async_remote_copy(
            src_ref=src, dst_ref=dst, send_sem=send, recv_sem=recv, device_id=peer,
            device_id_type=MESH,
        )

    def radial_copies(buffer, section, tile):
        where = pl.ds(PAD + TILE * tile, TILE)
        slot = (section * tiles + tile) * 2
        up = remote(
            buffer.at[:, pl.ds(rows, 2), where, :], buffer.at[:, pl.ds(0, 2), where, :],
            radial_send.at[slot], radial_recv.at[slot], radial_peer(1),
        )
        down = remote(
            buffer.at[:, pl.ds(2, 2), where, :], buffer.at[:, pl.ds(rows + 2, 2), where, :],
            radial_send.at[slot + 1], radial_recv.at[slot + 1], radial_peer(slabs - 1),
        )
        return up, down

    def radial_start(copies):
        up, down = copies

        @pl.when(has_up)
        def _():
            up.start()

        @pl.when(has_down)
        def _():
            down.start()

    def radial_sent(copies):
        up, down = copies

        @pl.when(has_up)
        def _():
            up.wait_send()

        @pl.when(has_down)
        def _():
            down.wait_send()

    def radial_land(copies, buffer, tile):
        up, down = copies
        where = pl.ds(PAD + TILE * tile, TILE)

        @pl.when(has_down)
        def _():
            up.wait_recv()

        @pl.when(jnp.logical_not(has_down))
        def _():
            value = buffer[:, 2, where, :]
            buffer[:, 0, where, :] = value
            buffer[:, 1, where, :] = value

        @pl.when(has_up)
        def _():
            down.wait_recv()

        @pl.when(jnp.logical_not(has_up))
        def _():
            value = buffer[:, rows + 1, where, :]
            buffer[:, rows + 2, where, :] = value
            buffer[:, rows + 3, where, :] = value

    whole, inside, low_edge, high_edge = (0, rows), (2, rows - 4), (0, 2), (rows - 2, 2)

    def phi_copies(section, piece, slot):
        where = pl.ds(*piece)
        return [
            remote(
                edge.at[section * 2 + side, :, where], halo.at[section * 2 + side, :, where],
                phi_send.at[slot + side], phi_recv.at[slot + side], phi_peer(jump),
            )
            for side, jump in ((0, wedges - 1), (1, 1))
        ]

    def phi_pack(buffer, section, side, piece):
        begin, count = piece
        start = PAD if side == 0 else PAD + cells - 2
        edge[section * 2 + side, :, pl.ds(begin, count)] = buffer[
            :, pl.ds(2 + begin, count), pl.ds(start, 2), :
        ]

    def phi_unpack(buffer, section, side, piece):
        begin, count = piece
        start = PAD + cells if side == 0 else PAD - 2
        buffer[:, pl.ds(2 + begin, count), pl.ds(start, 2), :] = halo[
            section * 2 + side, :, pl.ds(begin, count)
        ]

    shape = (TILE, lanes)
    lane = lax.broadcasted_iota(jnp.int32, (rows, lanes), 1)
    line = lax.broadcasted_iota(jnp.int32, (rows, lanes), 0)
    column = jnp.sum(first[0, pl.ds(2, rows), pl.ds(PAD, cells), :], axis=1)
    column = jnp.sum(column * table[0:1, :], axis=1, keepdims=True)
    centres = INNER_RADIUS + (
        (slab * rows + line).astype(jnp.float32) + 0.5
    ) * radial_step
    column = column * centres * centres * (radial_step * theta_step * phi_step)
    part[...] = jnp.sum(jnp.where(lane == line, column, 0.0), axis=0, keepdims=True)
    got[0] = part[...]
    phi_pack(first, 0, 0, whole)
    phi_pack(first, 0, 1, whole)
    pl.semaphore_wait(barrier, len(jumps))

    part_copies = []
    for i, j in jumps:
        slot = i * wedges + j
        part_copies.append(
            remote(part, got.at[slot], part_send.at[slot], part_recv.at[slot], peer_at((i, j)))
        )
    first_radial = [radial_copies(first, 0, t) for t in range(tiles)]
    second_radial = [radial_copies(second, 1, t) for t in range(tiles)]
    first_phi = phi_copies(0, whole, 0)
    inside_phi = phi_copies(1, inside, 2)
    low_phi, high_phi = phi_copies(1, low_edge, 4), phi_copies(1, high_edge, 6)
    for copy in first_phi + part_copies:
        copy.start()
    for t in range(tiles):
        radial_start(first_radial[t])

    lane_tile = lax.broadcasted_iota(jnp.int32, shape, 1)
    is_first, is_last = lane_tile == 0, lane_tile == lanes - 1

    def rate(buffer, r, tile, radial=True, rest=True):
        start = PAD + TILE * tile

        def at(row, offset):
            return [buffer[k, row + 2, pl.ds(start + offset, TILE), :] for k in range(variables)]

        def spread(value):
            return jnp.broadcast_to(value, shape)

        index = jnp.full(shape, slab * rows + r, jnp.int32).astype(jnp.float32)
        radius = INNER_RADIUS + (index + 0.5) * radial_step
        inner, outer = radius - 0.5 * radial_step, radius + 0.5 * radial_step
        inverse_r = 1.0 / radius
        centre = at(r, 0)
        total = [0.0] * variables
        if radial:
            lower, upper = two_faces([at(r + o, 0) if o else centre for o in range(-2, 3)], 1)
            scale = inverse_r * inverse_r * (1.0 / radial_step)
            area_in, area_out = inner * inner * scale, outer * outer * scale
            total = [area_in * a - area_out * b for a, b in zip(lower, upper)]
        if not rest:
            return total
        lower, upper = two_faces([at(r, o) if o else centre for o in range(-2, 3)], 3)
        around = inverse_r * spread(table[4:5, :])
        scale = around * (1.0 / phi_step)
        total = [t + (a - b) * scale for t, a, b in zip(total, lower, upper)]
        left, right = [], []
        for q in centre:
            after = jnp.where(is_last, q, pltpu.roll(q, lanes - 1, 1))
            above = after - q
            below = jnp.where(is_first, 0.0, pltpu.roll(above, 1, 1))
            slope = half_slope(below, above)
            left.append(q + slope)
            right.append(jnp.where(is_last, q, pltpu.roll(q - slope, lanes - 1, 1)))
        upper = flux(left, right, 2)
        scale = around * (1.0 / theta_step)
        low_sine, high_sine = spread(table[1:2, :]), spread(table[2:3, :])
        low_area, high_area = low_sine * scale, high_sine * scale
        total = [
            t + (low_area * pltpu.roll(f, 1, 1) - high_area * f) for t, f in zip(total, upper)
        ]
        density, inverse, pressure = thermo(centre)
        vr, vt, vp = (centre[m] * inverse for m in (1, 2, 3))
        cot = spread(table[3:4, :])
        total[1] = total[1] + (2.0 * pressure + density * (vt * vt + vp * vp)) * inverse_r
        total[2] = total[2] + (
            (pressure + density * vp * vp) * cot - density * vr * vt
        ) * inverse_r
        total[3] = total[3] - density * vp * (vr + vt * cot) * inverse_r
        return centre, density, total

    def gravity_at(r):
        return jnp.broadcast_to(pull[pl.ds(r, 1), :], shape)

    def with_gravity(rates, r):
        centre, density, total = rates
        gravity = gravity_at(r)
        total[1] = total[1] - density * gravity
        total[4] = total[4] - centre[1] * gravity
        return centre, total

    def section_one(r, tile):
        centre, _, total = rate(first, r, tile)
        where = pl.ds(PAD + TILE * tile, TILE)
        for k in range(variables):
            second[k, r + 2, where, :] = centre[k] + timestep * total[k]

    def rest_one(r, tile):
        centre, total = with_gravity(rate(first, r, tile, radial=False), r)
        where = pl.ds(PAD + TILE * tile, TILE)
        for k in range(variables):
            second[k, r + 2, where, :] = centre[k] + timestep * total[k]

    def radial_one(r, tile):
        total = rate(first, r, tile, rest=False)
        where = pl.ds(PAD + TILE * tile, TILE)
        for k in range(variables):
            second[k, r + 2, where, :] = second[k, r + 2, where, :] + timestep * total[k]

    def late_gravity(r, tile):
        where = pl.ds(PAD + TILE * tile, TILE)
        gravity = timestep * gravity_at(r)
        density = jnp.maximum(first[0, r + 2, where, :], MINIMUM_DENSITY)
        second[1, r + 2, where, :] = second[1, r + 2, where, :] - density * gravity
        second[4, r + 2, where, :] = (
            second[4, r + 2, where, :] - first[1, r + 2, where, :] * gravity
        )

    def section_two(r, tile, radial=True):
        centre, total = with_gravity(rate(second, r, tile, radial=radial), r)
        where = pl.ds(PAD + TILE * tile, TILE)
        into = pl.ds(TILE * tile, TILE)
        for k in range(variables):
            begin = first[k, r + 2, where, :]
            out_ref[k, r, into, :] = 0.5 * begin + 0.5 * (centre[k] + timestep * total[k])

    def radial_two(r, tile):
        total = rate(second, r, tile, rest=False)
        into = pl.ds(TILE * tile, TILE)
        for k in range(variables):
            out_ref[k, r, into, :] = out_ref[k, r, into, :] + (0.5 * timestep) * total[k]

    def each_row(low, high, step):
        lax.fori_loop(low, high, lambda r, _: (step(r), 0)[1], 0)

    def each_edge(step):
        lax.fori_loop(
            0, 4, lambda i, _: (step(i + (i // 2) * (rows - 4)), 0)[1], 0
        )

    def all_tiles(step):
        def run(r):
            for t in range(tiles):
                step(r, t)

        return run

    for side, copy in enumerate(first_phi):
        copy.wait_recv()
        phi_unpack(first, 0, side, whole)
    each_row(2, rows - 2, all_tiles(section_one))

    for copy in part_copies:
        copy.wait_recv()

    def slab_shells(jump):
        shells = jnp.zeros((1, lanes), jnp.float32)
        for w in range(wedges):
            shells = shells + got[jump * wedges + lax.rem(wedge + wedges - w, wedges)]
        return shells

    before = jnp.zeros((1, lanes), jnp.float32)
    for j in range(slabs - 1, 0, -1):
        before = before + jnp.where(slab >= j, slab_shells(j), 0.0)
    before = jnp.sum(before, axis=1, keepdims=True)
    weight = jnp.where(lane < line, 1.0, jnp.where(lane == line, 0.5, 0.0))
    within = jnp.sum(weight * slab_shells(0), axis=1, keepdims=True)
    enclosed = core[0] + before + within + jnp.zeros((rows, lanes), jnp.float32)
    mass_ref[...] = jnp.sum(jnp.where(lane == line, enclosed, 0.0), axis=0, keepdims=True)[:, :rows]
    pull[...] = strength * enclosed / (centres * centres)
    each_row(2, rows - 2, all_tiles(late_gravity))
    for side, copy in enumerate(inside_phi):
        phi_pack(second, 1, side, inside)
        copy.start()
    each_edge(all_tiles(rest_one))

    for t in range(tiles):
        radial_land(first_radial[t], first, t)
        each_edge(lambda r: radial_one(r, t))
        radial_start(second_radial[t])
        for side, last in ((0, 0), (1, tiles - 1)):
            if t == last:
                phi_pack(second, 1, side, low_edge)
                phi_pack(second, 1, side, high_edge)
                low_phi[side].start()
                high_phi[side].start()
        if t == 0:
            for side, copy in enumerate(inside_phi):
                copy.wait_recv()
                phi_unpack(second, 1, side, inside)
        each_row(2, rows - 2, lambda r: section_two(r, t))
    for side in range(2):
        low_phi[side].wait_recv()
        high_phi[side].wait_recv()
        phi_unpack(second, 1, side, low_edge)
        phi_unpack(second, 1, side, high_edge)
    each_edge(all_tiles(lambda r, t: section_two(r, t, False)))
    for t in range(tiles):
        radial_land(second_radial[t], second, t)
        each_edge(lambda r: radial_two(r, t))

    for copy in part_copies + first_phi + inside_phi + low_phi + high_phi:
        copy.wait_send()
    for copies in first_radial + second_radial:
        radial_sent(copies)


def body(conserved, core_mass):
    variables, rows, cells, lanes = conserved.shape
    slabs, wedges = lax.axis_size("radial"), lax.axis_size("phi")
    sizes = step_sizes(rows * slabs, cells * wedges, lanes)
    table = jnp.asarray(angle_tables(lanes, sizes[1]))
    tiles = cells // TILE
    padded = (variables, rows + 4, cells + 2 * PAD, lanes)
    vmem = pl.BlockSpec(memory_space=pltpu.VMEM)
    dma = pltpu.SemaphoreType.DMA
    advanced, mass = pl.pallas_call(
        functools.partial(kernel, sizes, (slabs, wedges)),
        out_shape=(
            pltpu.VMEM(conserved.shape, jnp.float32),
            pltpu.VMEM((1, rows), jnp.float32),
        ),
        in_specs=[pl.BlockSpec(memory_space=pl.ANY)] * 3,
        out_specs=(vmem, vmem),
        scratch_shapes=[
            pltpu.VMEM(padded, jnp.float32),
            pltpu.VMEM(padded, jnp.float32),
            pltpu.VMEM((4, variables, rows, 2, lanes), jnp.float32),
            pltpu.VMEM((4, variables, rows, 2, lanes), jnp.float32),
            pltpu.VMEM((1, lanes), jnp.float32),
            pltpu.VMEM((slabs * wedges, 1, lanes), jnp.float32),
            pltpu.VMEM((rows, lanes), jnp.float32),
            pltpu.VMEM((TILE, lanes), jnp.float32),
            pltpu.SMEM((1,), jnp.float32),
            dma((3,)),
            dma((4 * tiles,)),
            dma((4 * tiles,)),
            dma((8,)),
            dma((8,)),
            dma((slabs * wedges,)),
            dma((slabs * wedges,)),
        ],
        compiler_params=pltpu.CompilerParams(collective_id=0, has_side_effects=True),
    )(core_mass, table, conserved)
    return advanced, mass.reshape(rows)


def solution(mesh):
    in_specs = (P(None, "radial", "phi", None), P())
    out_specs = (P(None, "radial", "phi", None), P("radial"))
    return jax.shard_map(body, mesh=mesh, in_specs=in_specs, out_specs=out_specs, check_vma=False)
```

```python
import functools
import math

import jax
import jax.numpy as jnp
import numpy as np
from jax import lax
from jax.experimental import pallas as pl
from jax.experimental.pallas import tpu as pltpu
from jax.sharding import PartitionSpec as P

ADIABATIC = 4.0 / 3.0
INNER_RADIUS = 1.0
OUTER_RADIUS = 2.0
COURANT = 0.4
GRAVITY_KICK = 0.004
MINIMUM_DENSITY = 0.05
PRESSURE_FLOOR = 0.01
MESH = pl.DeviceIdType.MESH
TILE = 8
PAD = 8


def step_sizes(radial_total, phi_total, theta_total):
    theta_step = math.pi / theta_total
    phi_step = 2.0 * math.pi / phi_total
    polar_width = INNER_RADIUS * math.sin(0.5 * theta_step) * phi_step
    radial_step = min(2.0 * polar_width, (OUTER_RADIUS - INNER_RADIUS) / radial_total)
    timestep = COURANT * min(radial_step, polar_width)
    return (radial_step, theta_step, phi_step, timestep)


def angle_tables(theta_cells, theta_step):
    step = np.float32(theta_step)
    centre = (np.arange(theta_cells, dtype=np.float32) + np.float32(0.5)) * step
    face = np.arange(theta_cells + 1, dtype=np.float32) * step
    sine = np.sin(centre.astype(np.float64))
    cosine = np.cos(centre.astype(np.float64))
    face_sine = np.sin(face.astype(np.float64))
    zero = np.zeros(theta_cells)
    rows = [sine, face_sine[:-1], face_sine[1:], cosine / sine, 1.0 / sine, zero, zero, zero]
    return np.stack(rows).astype(np.float32)


def half_slope(below, above):
    return 0.5 * (
        jnp.maximum(jnp.minimum(below, above), 0.0) + jnp.minimum(jnp.maximum(below, above), 0.0)
    )


def thermo(q):
    density = jnp.maximum(q[0], MINIMUM_DENSITY)
    inverse = 1.0 / density
    kinetic = 0.5 * (q[1] * q[1] + q[2] * q[2] + q[3] * q[3]) * inverse
    pressure = jnp.maximum((ADIABATIC - 1.0) * (q[4] - kinetic), PRESSURE_FLOOR * density)
    return density, inverse, pressure


def physical(q, component):
    _, inverse, pressure = thermo(q)
    normal = q[component] * inverse
    squared = ADIABATIC * pressure * inverse
    return normal, pressure, jnp.abs(normal) + squared * lax.rsqrt(squared)


def flux(left, right, component):
    left_v, left_p, left_a = physical(left, component)
    right_v, right_p, right_a = physical(right, component)
    signal = jnp.maximum(left_a, right_a)
    left_w = 0.5 * (left_v + signal)
    right_w = 0.5 * (right_v - signal)
    out = [a * left_w + b * right_w for a, b in zip(left, right)]
    out[component] = out[component] + 0.5 * (left_p + right_p)
    out[4] = out[4] + 0.5 * (left_p * left_v + right_p * right_v)
    return out


def two_faces(rows, component):
    lower_left, lower_right, upper_left, upper_right = [], [], [], []
    for a, b, c, d, e in zip(*rows):
        ab, bc, cd, de = b - a, c - b, d - c, e - d
        sb, sc, sd = half_slope(ab, bc), half_slope(bc, cd), half_slope(cd, de)
        lower_left.append(b + sb)
        lower_right.append(c - sc)
        upper_left.append(c + sc)
        upper_right.append(d - sd)
    return flux(lower_left, lower_right, component), flux(upper_left, upper_right, component)


def kernel(
    sizes,
    counts,
    core_ref,
    table_ref,
    input_ref,
    out_ref,
    mass_ref,
    first,
    second,
    edge,
    halo,
    part,
    slab_part,
    got,
    pull,
    table,
    core,
    load_sem,
    radial_send,
    radial_recv,
    phi_send,
    phi_recv,
    part_send,
    part_recv,
):
    radial_step, theta_step, phi_step, timestep = sizes
    slabs, wedges = counts
    variables, rows, cells, lanes = input_ref.shape
    tiles = cells // TILE
    strength = GRAVITY_KICK / timestep
    slab, wedge = lax.axis_index("radial"), lax.axis_index("phi")
    has_up, has_down = slab < slabs - 1, slab > 0

    load = pltpu.make_async_copy(
        input_ref, first.at[:, pl.ds(2, rows), pl.ds(PAD, cells), :], load_sem.at[0]
    )
    load.start()
    load_table = pltpu.make_async_copy(table_ref, table, load_sem.at[1])
    load_table.start()
    load_core = pltpu.make_async_copy(core_ref, core, load_sem.at[2])
    load_core.start()

    def radial_peer(jump):
        return (lax.rem(slab + jump, slabs), wedge)

    def phi_peer(jump):
        return (slab, lax.rem(wedge + jump, wedges))

    barrier = pltpu.get_barrier_semaphore()
    jumps = [(i, 0) for i in range(1, slabs)] + [(0, j) for j in range(1, wedges)]

    def peer_at(jump):
        return (radial_peer(jump[0])[0], phi_peer(jump[1])[1])

    for jump in jumps:
        pl.semaphore_signal(barrier, inc=1, device_id=peer_at(jump), device_id_type=MESH)
    load.wait()
    load_table.wait()
    load_core.wait()

    def remote(src, dst, send, recv, peer):
        return pltpu.make_async_remote_copy(
            src_ref=src, dst_ref=dst, send_sem=send, recv_sem=recv, device_id=peer,
            device_id_type=MESH,
        )

    def radial_copies(buffer, section, tile):
        where = pl.ds(PAD + TILE * tile, TILE)
        slot = (section * tiles + tile) * 2
        up = remote(
            buffer.at[:, pl.ds(rows, 2), where, :], buffer.at[:, pl.ds(0, 2), where, :],
            radial_send.at[slot], radial_recv.at[slot], radial_peer(1),
        )
        down = remote(
            buffer.at[:, pl.ds(2, 2), where, :], buffer.at[:, pl.ds(rows + 2, 2), where, :],
            radial_send.at[slot + 1], radial_recv.at[slot + 1], radial_peer(slabs - 1),
        )
        return up, down

    def radial_start(copies):
        up, down = copies

        @pl.when(has_up)
        def _():
            up.start()

        @pl.when(has_down)
        def _():
            down.start()

    def radial_sent(copies):
        up, down = copies

        @pl.when(has_up)
        def _():
            up.wait_send()

        @pl.when(has_down)
        def _():
            down.wait_send()

    def radial_land(copies, buffer, tile):
        up, down = copies
        where = pl.ds(PAD + TILE * tile, TILE)

        @pl.when(has_down)
        def _():
            up.wait_recv()

        @pl.when(jnp.logical_not(has_down))
        def _():
            value = buffer[:, 2, where, :]
            buffer[:, 0, where, :] = value
            buffer[:, 1, where, :] = value

        @pl.when(has_up)
        def _():
            down.wait_recv()

        @pl.when(jnp.logical_not(has_up))
        def _():
            value = buffer[:, rows + 1, where, :]
            buffer[:, rows + 2, where, :] = value
            buffer[:, rows + 3, where, :] = value

    whole, inside, low_edge, high_edge = (0, rows), (2, rows - 4), (0, 2), (rows - 2, 2)

    def phi_copies(section, piece, slot):
        where = pl.ds(*piece)
        return [
            remote(
                edge.at[section * 2 + side, :, where], halo.at[section * 2 + side, :, where],
                phi_send.at[slot + side], phi_recv.at[slot + side], phi_peer(jump),
            )
            for side, jump in ((0, wedges - 1), (1, 1))
        ]

    def phi_pack(buffer, section, side, piece):
        begin, count = piece
        start = PAD if side == 0 else PAD + cells - 2
        edge[section * 2 + side, :, pl.ds(begin, count)] = buffer[
            :, pl.ds(2 + begin, count), pl.ds(start, 2), :
        ]

    def phi_unpack(buffer, section, side, piece):
        begin, count = piece
        start = PAD + cells if side == 0 else PAD - 2
        buffer[:, pl.ds(2 + begin, count), pl.ds(start, 2), :] = halo[
            section * 2 + side, :, pl.ds(begin, count)
        ]

    shape = (TILE, lanes)
    lane = lax.broadcasted_iota(jnp.int32, (rows, lanes), 1)
    line = lax.broadcasted_iota(jnp.int32, (rows, lanes), 0)
    column = jnp.sum(first[0, pl.ds(2, rows), pl.ds(PAD, cells), :], axis=1)
    column = jnp.sum(column * table[0:1, :], axis=1, keepdims=True)
    centres = INNER_RADIUS + (
        (slab * rows + line).astype(jnp.float32) + 0.5
    ) * radial_step
    column = column * centres * centres * (radial_step * theta_step * phi_step)
    part[...] = jnp.sum(jnp.where(lane == line, column, 0.0), axis=0, keepdims=True)
    got[0] = part[...]
    phi_pack(first, 0, 0, whole)
    phi_pack(first, 0, 1, whole)
    pl.semaphore_wait(barrier, len(jumps))

    def wedge_sum():
        shells = jnp.zeros((1, lanes), jnp.float32)
        for w in range(wedges):
            shells = shells + got[lax.rem(wedge + wedges - w, wedges)]
        return shells

    part_copies = []
    for j in range(1, wedges):
        i, slot = 0, j
        part_copies.append(
            remote(part, got.at[slot], part_send.at[slot], part_recv.at[slot], peer_at((i, j)))
        )
    first_radial = [radial_copies(first, 0, t) for t in range(tiles)]
    second_radial = [radial_copies(second, 1, t) for t in range(tiles)]
    first_phi = phi_copies(0, whole, 0)
    inside_phi = phi_copies(1, inside, 2)
    low_phi, high_phi = phi_copies(1, low_edge, 4), phi_copies(1, high_edge, 6)
    for copy in part_copies + first_phi:
        copy.start()
    radial_start(first_radial[0])
    for copy in part_copies:
        copy.wait_recv()
    slab_part[...] = wedge_sum()
    slab_copies = []
    for j in range(1, slabs):
        slot = j * wedges
        slab_copies.append(
            remote(
                slab_part, got.at[slot], part_send.at[slot], part_recv.at[slot], radial_peer(j)
            )
        )
    for copy in slab_copies:
        copy.start()
    for t in range(1, tiles):
        radial_start(first_radial[t])

    lane_tile = lax.broadcasted_iota(jnp.int32, shape, 1)
    is_first, is_last = lane_tile == 0, lane_tile == lanes - 1

    def rate(buffer, r, tile, radial=True, rest=True):
        start = PAD + TILE * tile

        def at(row, offset):
            return [buffer[k, row + 2, pl.ds(start + offset, TILE), :] for k in range(variables)]

        def spread(value):
            return jnp.broadcast_to(value, shape)

        index = jnp.full(shape, slab * rows + r, jnp.int32).astype(jnp.float32)
        radius = INNER_RADIUS + (index + 0.5) * radial_step
        inner, outer = radius - 0.5 * radial_step, radius + 0.5 * radial_step
        inverse_r = 1.0 / radius
        centre = at(r, 0)
        total = [0.0] * variables
        if radial:
            lower, upper = two_faces([at(r + o, 0) if o else centre for o in range(-2, 3)], 1)
            scale = inverse_r * inverse_r * (1.0 / radial_step)
            area_in, area_out = inner * inner * scale, outer * outer * scale
            total = [area_in * a - area_out * b for a, b in zip(lower, upper)]
        if not rest:
            return total
        lower, upper = two_faces([at(r, o) if o else centre for o in range(-2, 3)], 3)
        around = inverse_r * spread(table[4:5, :])
        scale = around * (1.0 / phi_step)
        total = [t + (a - b) * scale for t, a, b in zip(total, lower, upper)]
        left, right = [], []
        for q in centre:
            after = jnp.where(is_last, q, pltpu.roll(q, lanes - 1, 1))
            above = after - q
            below = jnp.where(is_first, 0.0, pltpu.roll(above, 1, 1))
            slope = half_slope(below, above)
            left.append(q + slope)
            right.append(jnp.where(is_last, q, pltpu.roll(q - slope, lanes - 1, 1)))
        upper = flux(left, right, 2)
        scale = around * (1.0 / theta_step)
        low_sine, high_sine = spread(table[1:2, :]), spread(table[2:3, :])
        low_area, high_area = low_sine * scale, high_sine * scale
        total = [
            t + (low_area * pltpu.roll(f, 1, 1) - high_area * f) for t, f in zip(total, upper)
        ]
        density, inverse, pressure = thermo(centre)
        vr, vt, vp = (centre[m] * inverse for m in (1, 2, 3))
        cot = spread(table[3:4, :])
        total[1] = total[1] + (2.0 * pressure + density * (vt * vt + vp * vp)) * inverse_r
        total[2] = total[2] + (
            (pressure + density * vp * vp) * cot - density * vr * vt
        ) * inverse_r
        total[3] = total[3] - density * vp * (vr + vt * cot) * inverse_r
        return centre, density, total

    def gravity_at(r):
        return jnp.broadcast_to(pull[pl.ds(r, 1), :], shape)

    def with_gravity(rates, r):
        centre, density, total = rates
        gravity = gravity_at(r)
        total[1] = total[1] - density * gravity
        total[4] = total[4] - centre[1] * gravity
        return centre, total

    def section_one(r, tile):
        centre, _, total = rate(first, r, tile)
        where = pl.ds(PAD + TILE * tile, TILE)
        for k in range(variables):
            second[k, r + 2, where, :] = centre[k] + timestep * total[k]

    def rest_one(r, tile):
        centre, total = with_gravity(rate(first, r, tile, radial=False), r)
        where = pl.ds(PAD + TILE * tile, TILE)
        for k in range(variables):
            second[k, r + 2, where, :] = centre[k] + timestep * total[k]

    def radial_one(r, tile):
        total = rate(first, r, tile, rest=False)
        where = pl.ds(PAD + TILE * tile, TILE)
        for k in range(variables):
            second[k, r + 2, where, :] = second[k, r + 2, where, :] + timestep * total[k]

    def late_gravity(r, tile):
        where = pl.ds(PAD + TILE * tile, TILE)
        gravity = timestep * gravity_at(r)
        density = jnp.maximum(first[0, r + 2, where, :], MINIMUM_DENSITY)
        second[1, r + 2, where, :] = second[1, r + 2, where, :] - density * gravity
        second[4, r + 2, where, :] = (
            second[4, r + 2, where, :] - first[1, r + 2, where, :] * gravity
        )

    def section_two(r, tile, radial=True):
        centre, total = with_gravity(rate(second, r, tile, radial=radial), r)
        where = pl.ds(PAD + TILE * tile, TILE)
        into = pl.ds(TILE * tile, TILE)
        for k in range(variables):
            begin = first[k, r + 2, where, :]
            out_ref[k, r, into, :] = 0.5 * begin + 0.5 * (centre[k] + timestep * total[k])

    def radial_two(r, tile):
        total = rate(second, r, tile, rest=False)
        into = pl.ds(TILE * tile, TILE)
        for k in range(variables):
            out_ref[k, r, into, :] = out_ref[k, r, into, :] + (0.5 * timestep) * total[k]

    def each_row(low, high, step):
        lax.fori_loop(low, high, lambda r, _: (step(r), 0)[1], 0)

    def each_edge(step):
        lax.fori_loop(
            0, 4, lambda i, _: (step(i + (i // 2) * (rows - 4)), 0)[1], 0
        )

    def all_tiles(step):
        def run(r):
            for t in range(tiles):
                step(r, t)

        return run

    for side, copy in enumerate(first_phi):
        copy.wait_recv()
        phi_unpack(first, 0, side, whole)
    each_row(2, rows - 2, all_tiles(section_one))

    for copy in slab_copies:
        copy.wait_recv()
    before = jnp.zeros((1, lanes), jnp.float32)
    for j in range(slabs - 1, 0, -1):
        before = before + jnp.where(slab >= j, got[j * wedges], 0.0)
    before = jnp.sum(before, axis=1, keepdims=True)
    weight = jnp.where(lane < line, 1.0, jnp.where(lane == line, 0.5, 0.0))
    within = jnp.sum(weight * slab_part[...], axis=1, keepdims=True)
    enclosed = core[0] + before + within + jnp.zeros((rows, lanes), jnp.float32)
    mass_ref[...] = jnp.sum(jnp.where(lane == line, enclosed, 0.0), axis=0, keepdims=True)[:, :rows]
    pull[...] = strength * enclosed / (centres * centres)
    each_row(2, rows - 2, all_tiles(late_gravity))
    for side, copy in enumerate(inside_phi):
        phi_pack(second, 1, side, inside)
        copy.start()
    each_edge(all_tiles(rest_one))

    for t in range(tiles):
        radial_land(first_radial[t], first, t)
        each_edge(lambda r: radial_one(r, t))
        radial_start(second_radial[t])
        for side, last in ((0, 0), (1, tiles - 1)):
            if t == last:
                phi_pack(second, 1, side, low_edge)
                phi_pack(second, 1, side, high_edge)
                low_phi[side].start()
                high_phi[side].start()
        if t == 0:
            for side, copy in enumerate(inside_phi):
                copy.wait_recv()
                phi_unpack(second, 1, side, inside)
        each_row(2, rows - 2, lambda r: section_two(r, t))
    for side in range(2):
        low_phi[side].wait_recv()
        high_phi[side].wait_recv()
        phi_unpack(second, 1, side, low_edge)
        phi_unpack(second, 1, side, high_edge)
    each_edge(all_tiles(lambda r, t: section_two(r, t, False)))
    for t in range(tiles):
        radial_land(second_radial[t], second, t)
        each_edge(lambda r: radial_two(r, t))

    for copy in part_copies + slab_copies + first_phi + inside_phi + low_phi + high_phi:
        copy.wait_send()
    for copies in first_radial + second_radial:
        radial_sent(copies)


def body(conserved, core_mass):
    variables, rows, cells, lanes = conserved.shape
    slabs, wedges = lax.axis_size("radial"), lax.axis_size("phi")
    sizes = step_sizes(rows * slabs, cells * wedges, lanes)
    table = jnp.asarray(angle_tables(lanes, sizes[1]))
    tiles = cells // TILE
    padded = (variables, rows + 4, cells + 2 * PAD, lanes)
    vmem = pl.BlockSpec(memory_space=pltpu.VMEM)
    dma = pltpu.SemaphoreType.DMA
    advanced, mass = pl.pallas_call(
        functools.partial(kernel, sizes, (slabs, wedges)),
        out_shape=(
            pltpu.VMEM(conserved.shape, jnp.float32),
            pltpu.VMEM((1, rows), jnp.float32),
        ),
        in_specs=[pl.BlockSpec(memory_space=pl.ANY)] * 3,
        out_specs=(vmem, vmem),
        scratch_shapes=[
            pltpu.VMEM(padded, jnp.float32),
            pltpu.VMEM(padded, jnp.float32),
            pltpu.VMEM((4, variables, rows, 2, lanes), jnp.float32),
            pltpu.VMEM((4, variables, rows, 2, lanes), jnp.float32),
            pltpu.VMEM((1, lanes), jnp.float32),
            pltpu.VMEM((1, lanes), jnp.float32),
            pltpu.VMEM((slabs * wedges, 1, lanes), jnp.float32),
            pltpu.VMEM((rows, lanes), jnp.float32),
            pltpu.VMEM((TILE, lanes), jnp.float32),
            pltpu.SMEM((1,), jnp.float32),
            dma((3,)),
            dma((4 * tiles,)),
            dma((4 * tiles,)),
            dma((8,)),
            dma((8,)),
            dma((slabs * wedges,)),
            dma((slabs * wedges,)),
        ],
        compiler_params=pltpu.CompilerParams(collective_id=0, has_side_effects=True),
    )(core_mass, table, conserved)
    return advanced, mass.reshape(rows)


def solution(mesh):
    in_specs = (P(None, "radial", "phi", None), P())
    out_specs = (P(None, "radial", "phi", None), P("radial"))
    return jax.shard_map(body, mesh=mesh, in_specs=in_specs, out_specs=out_specs, check_vma=False)
```

```python
import functools
import math

import jax
import jax.numpy as jnp
import numpy as np
from jax import lax
from jax.experimental import pallas as pl
from jax.experimental.pallas import tpu as pltpu
from jax.sharding import PartitionSpec as P

ADIABATIC = 4.0 / 3.0
INNER_RADIUS = 1.0
OUTER_RADIUS = 2.0
COURANT = 0.4
GRAVITY_KICK = 0.004
MINIMUM_DENSITY = 0.05
PRESSURE_FLOOR = 0.01
MESH = pl.DeviceIdType.MESH
TILE = 8
PAD = 8


def step_sizes(radial_total, phi_total, theta_total):
    theta_step = math.pi / theta_total
    phi_step = 2.0 * math.pi / phi_total
    polar_width = INNER_RADIUS * math.sin(0.5 * theta_step) * phi_step
    radial_step = min(2.0 * polar_width, (OUTER_RADIUS - INNER_RADIUS) / radial_total)
    timestep = COURANT * min(radial_step, polar_width)
    return (radial_step, theta_step, phi_step, timestep)


def angle_tables(theta_cells, theta_step):
    step = np.float32(theta_step)
    centre = (np.arange(theta_cells, dtype=np.float32) + np.float32(0.5)) * step
    face = np.arange(theta_cells + 1, dtype=np.float32) * step
    sine = np.sin(centre.astype(np.float64))
    cosine = np.cos(centre.astype(np.float64))
    face_sine = np.sin(face.astype(np.float64))
    zero = np.zeros(theta_cells)
    rows = [sine, face_sine[:-1], face_sine[1:], cosine / sine, 1.0 / sine, zero, zero, zero]
    return np.stack(rows).astype(np.float32)


def half_slope(below, above):
    return 0.5 * (
        jnp.maximum(jnp.minimum(below, above), 0.0) + jnp.minimum(jnp.maximum(below, above), 0.0)
    )


def thermo(q):
    density = jnp.maximum(q[0], MINIMUM_DENSITY)
    inverse = 1.0 / density
    kinetic = 0.5 * (q[1] * q[1] + q[2] * q[2] + q[3] * q[3]) * inverse
    pressure = jnp.maximum((ADIABATIC - 1.0) * (q[4] - kinetic), PRESSURE_FLOOR * density)
    return density, inverse, pressure


def physical(q, component):
    _, inverse, pressure = thermo(q)
    normal = q[component] * inverse
    squared = ADIABATIC * pressure * inverse
    return normal, pressure, jnp.abs(normal) + squared * lax.rsqrt(squared)


def flux(left, right, component):
    left_v, left_p, left_a = physical(left, component)
    right_v, right_p, right_a = physical(right, component)
    signal = jnp.maximum(left_a, right_a)
    left_w = 0.5 * (left_v + signal)
    right_w = 0.5 * (right_v - signal)
    out = [a * left_w + b * right_w for a, b in zip(left, right)]
    out[component] = out[component] + 0.5 * (left_p + right_p)
    out[4] = out[4] + 0.5 * (left_p * left_v + right_p * right_v)
    return out


def two_faces(rows, component):
    lower_left, lower_right, upper_left, upper_right = [], [], [], []
    for a, b, c, d, e in zip(*rows):
        ab, bc, cd, de = b - a, c - b, d - c, e - d
        sb, sc, sd = half_slope(ab, bc), half_slope(bc, cd), half_slope(cd, de)
        lower_left.append(b + sb)
        lower_right.append(c - sc)
        upper_left.append(c + sc)
        upper_right.append(d - sd)
    return flux(lower_left, lower_right, component), flux(upper_left, upper_right, component)


def kernel(
    sizes,
    counts,
    core_ref,
    table_ref,
    input_ref,
    out_ref,
    mass_ref,
    first,
    second,
    edge,
    halo,
    part,
    slab_part,
    got,
    pull,
    table,
    core,
    load_sem,
    radial_send,
    radial_recv,
    phi_send,
    phi_recv,
    part_send,
    part_recv,
):
    radial_step, theta_step, phi_step, timestep = sizes
    slabs, wedges = counts
    variables, rows, cells, lanes = input_ref.shape
    tiles = cells // TILE
    strength = GRAVITY_KICK / timestep
    slab, wedge = lax.axis_index("radial"), lax.axis_index("phi")
    has_up, has_down = slab < slabs - 1, slab > 0

    load = pltpu.make_async_copy(
        input_ref, first.at[:, pl.ds(2, rows), pl.ds(PAD, cells), :], load_sem.at[0]
    )
    load.start()
    load_table = pltpu.make_async_copy(table_ref, table, load_sem.at[1])
    load_table.start()
    load_core = pltpu.make_async_copy(core_ref, core, load_sem.at[2])
    load_core.start()

    def radial_peer(jump):
        return (lax.rem(slab + jump, slabs), wedge)

    def phi_peer(jump):
        return (slab, lax.rem(wedge + jump, wedges))

    barrier = pltpu.get_barrier_semaphore()
    jumps = [(i, 0) for i in range(1, slabs)] + [(0, j) for j in range(1, wedges)]

    def peer_at(jump):
        return (radial_peer(jump[0])[0], phi_peer(jump[1])[1])

    for jump in jumps:
        pl.semaphore_signal(barrier, inc=1, device_id=peer_at(jump), device_id_type=MESH)
    load.wait()
    load_table.wait()
    load_core.wait()

    def remote(src, dst, send, recv, peer):
        return pltpu.make_async_remote_copy(
            src_ref=src, dst_ref=dst, send_sem=send, recv_sem=recv, device_id=peer,
            device_id_type=MESH,
        )

    def radial_copies(buffer, section, tile):
        where = pl.ds(PAD + TILE * tile, TILE)
        slot = (section * tiles + tile) * 2
        up = remote(
            buffer.at[:, pl.ds(rows, 2), where, :], buffer.at[:, pl.ds(0, 2), where, :],
            radial_send.at[slot], radial_recv.at[slot], radial_peer(1),
        )
        down = remote(
            buffer.at[:, pl.ds(2, 2), where, :], buffer.at[:, pl.ds(rows + 2, 2), where, :],
            radial_send.at[slot + 1], radial_recv.at[slot + 1], radial_peer(slabs - 1),
        )
        return up, down

    def radial_start(copies):
        up, down = copies

        @pl.when(has_up)
        def _():
            up.start()

        @pl.when(has_down)
        def _():
            down.start()

    def radial_sent(copies):
        up, down = copies

        @pl.when(has_up)
        def _():
            up.wait_send()

        @pl.when(has_down)
        def _():
            down.wait_send()

    def radial_land(copies, buffer, tile):
        up, down = copies
        where = pl.ds(PAD + TILE * tile, TILE)

        @pl.when(has_down)
        def _():
            up.wait_recv()

        @pl.when(jnp.logical_not(has_down))
        def _():
            value = buffer[:, 2, where, :]
            buffer[:, 0, where, :] = value
            buffer[:, 1, where, :] = value

        @pl.when(has_up)
        def _():
            down.wait_recv()

        @pl.when(jnp.logical_not(has_up))
        def _():
            value = buffer[:, rows + 1, where, :]
            buffer[:, rows + 2, where, :] = value
            buffer[:, rows + 3, where, :] = value

    whole, inside, low_edge, high_edge = (0, rows), (2, rows - 4), (0, 2), (rows - 2, 2)

    def phi_copies(section, piece, slot):
        where = pl.ds(*piece)
        return [
            remote(
                edge.at[section * 2 + side, :, where], halo.at[section * 2 + side, :, where],
                phi_send.at[slot + side], phi_recv.at[slot + side], phi_peer(jump),
            )
            for side, jump in ((0, wedges - 1), (1, 1))
        ]

    def phi_pack(buffer, section, side, piece):
        begin, count = piece
        start = PAD if side == 0 else PAD + cells - 2
        edge[section * 2 + side, :, pl.ds(begin, count)] = buffer[
            :, pl.ds(2 + begin, count), pl.ds(start, 2), :
        ]

    def phi_unpack(buffer, section, side, piece):
        begin, count = piece
        start = PAD + cells if side == 0 else PAD - 2
        buffer[:, pl.ds(2 + begin, count), pl.ds(start, 2), :] = halo[
            section * 2 + side, :, pl.ds(begin, count)
        ]

    shape = (TILE, lanes)
    lane = lax.broadcasted_iota(jnp.int32, (rows, lanes), 1)
    line = lax.broadcasted_iota(jnp.int32, (rows, lanes), 0)
    column = jnp.sum(first[0, pl.ds(2, rows), pl.ds(PAD, cells), :], axis=1)
    column = jnp.sum(column * table[0:1, :], axis=1, keepdims=True)
    centres = INNER_RADIUS + (
        (slab * rows + line).astype(jnp.float32) + 0.5
    ) * radial_step
    column = column * centres * centres * (radial_step * theta_step * phi_step)
    part[...] = jnp.sum(jnp.where(lane == line, column, 0.0), axis=0, keepdims=True)
    got[0] = part[...]
    phi_pack(first, 0, 0, whole)
    phi_pack(first, 0, 1, whole)
    pl.semaphore_wait(barrier, len(jumps))

    def wedge_sum():
        shells = jnp.zeros((1, lanes), jnp.float32)
        for w in range(wedges):
            shells = shells + got[lax.rem(wedge + wedges - w, wedges)]
        return shells

    part_copies = []
    for j in range(1, wedges):
        i, slot = 0, j
        part_copies.append(
            remote(part, got.at[slot], part_send.at[slot], part_recv.at[slot], peer_at((i, j)))
        )
    first_radial = [radial_copies(first, 0, t) for t in range(tiles)]
    second_radial = [radial_copies(second, 1, t) for t in range(tiles)]
    first_phi = phi_copies(0, whole, 0)
    inside_phi = phi_copies(1, inside, 2)
    low_phi, high_phi = phi_copies(1, low_edge, 4), phi_copies(1, high_edge, 6)
    for copy in part_copies + first_phi:
        copy.start()
    radial_start(first_radial[0])
    for copy in part_copies:
        copy.wait_recv()
    slab_part[...] = wedge_sum()
    slab_copies = []
    for j in range(1, slabs):
        slot = j * wedges
        slab_copies.append(
            remote(
                slab_part, got.at[slot], part_send.at[slot], part_recv.at[slot], radial_peer(j)
            )
        )
    for copy in slab_copies:
        copy.start()
    for t in range(1, tiles):
        radial_start(first_radial[t])

    lane_tile = lax.broadcasted_iota(jnp.int32, shape, 1)
    is_first, is_last = lane_tile == 0, lane_tile == lanes - 1

    def rate(buffer, r, tile, radial=True, rest=True):
        start = PAD + TILE * tile

        def at(row, offset):
            return [buffer[k, row + 2, pl.ds(start + offset, TILE), :] for k in range(variables)]

        def spread(value):
            return jnp.broadcast_to(value, shape)

        index = jnp.full(shape, slab * rows + r, jnp.int32).astype(jnp.float32)
        radius = INNER_RADIUS + (index + 0.5) * radial_step
        inner, outer = radius - 0.5 * radial_step, radius + 0.5 * radial_step
        inverse_r = 1.0 / radius
        centre = at(r, 0)
        total = [0.0] * variables
        if radial:
            lower, upper = two_faces([at(r + o, 0) if o else centre for o in range(-2, 3)], 1)
            scale = inverse_r * inverse_r * (1.0 / radial_step)
            area_in, area_out = inner * inner * scale, outer * outer * scale
            total = [area_in * a - area_out * b for a, b in zip(lower, upper)]
        if not rest:
            return total
        lower, upper = two_faces([at(r, o) if o else centre for o in range(-2, 3)], 3)
        around = inverse_r * spread(table[4:5, :])
        scale = around * (1.0 / phi_step)
        total = [t + (a - b) * scale for t, a, b in zip(total, lower, upper)]
        left, right = [], []
        for q in centre:
            after = jnp.where(is_last, q, pltpu.roll(q, lanes - 1, 1))
            above = after - q
            below = jnp.where(is_first, 0.0, pltpu.roll(above, 1, 1))
            slope = half_slope(below, above)
            left.append(q + slope)
            right.append(jnp.where(is_last, q, pltpu.roll(q - slope, lanes - 1, 1)))
        upper = flux(left, right, 2)
        scale = around * (1.0 / theta_step)
        low_sine, high_sine = spread(table[1:2, :]), spread(table[2:3, :])
        low_area, high_area = low_sine * scale, high_sine * scale
        total = [
            t + (low_area * pltpu.roll(f, 1, 1) - high_area * f) for t, f in zip(total, upper)
        ]
        density, inverse, pressure = thermo(centre)
        vr, vt, vp = (centre[m] * inverse for m in (1, 2, 3))
        cot = spread(table[3:4, :])
        total[1] = total[1] + (2.0 * pressure + density * (vt * vt + vp * vp)) * inverse_r
        total[2] = total[2] + (
            (pressure + density * vp * vp) * cot - density * vr * vt
        ) * inverse_r
        total[3] = total[3] - density * vp * (vr + vt * cot) * inverse_r
        return centre, density, total

    def gravity_at(r):
        return jnp.broadcast_to(pull[pl.ds(r, 1), :], shape)

    def with_gravity(rates, r):
        centre, density, total = rates
        gravity = gravity_at(r)
        total[1] = total[1] - density * gravity
        total[4] = total[4] - centre[1] * gravity
        return centre, total

    def section_one(r, tile):
        centre, _, total = rate(first, r, tile)
        where = pl.ds(PAD + TILE * tile, TILE)
        for k in range(variables):
            second[k, r + 2, where, :] = centre[k] + timestep * total[k]

    def rest_one(r, tile):
        centre, _, total = rate(first, r, tile, radial=False)
        where = pl.ds(PAD + TILE * tile, TILE)
        for k in range(variables):
            second[k, r + 2, where, :] = centre[k] + timestep * total[k]

    def radial_one(r, tile):
        total = rate(first, r, tile, rest=False)
        where = pl.ds(PAD + TILE * tile, TILE)
        for k in range(variables):
            second[k, r + 2, where, :] = second[k, r + 2, where, :] + timestep * total[k]

    def late_gravity(r, tile):
        where = pl.ds(PAD + TILE * tile, TILE)
        gravity = timestep * gravity_at(r)
        density = jnp.maximum(first[0, r + 2, where, :], MINIMUM_DENSITY)
        second[1, r + 2, where, :] = second[1, r + 2, where, :] - density * gravity
        second[4, r + 2, where, :] = (
            second[4, r + 2, where, :] - first[1, r + 2, where, :] * gravity
        )

    def section_two(r, tile, radial=True):
        centre, total = with_gravity(rate(second, r, tile, radial=radial), r)
        where = pl.ds(PAD + TILE * tile, TILE)
        into = pl.ds(TILE * tile, TILE)
        for k in range(variables):
            begin = first[k, r + 2, where, :]
            out_ref[k, r, into, :] = 0.5 * begin + 0.5 * (centre[k] + timestep * total[k])

    def radial_two(r, tile):
        total = rate(second, r, tile, rest=False)
        into = pl.ds(TILE * tile, TILE)
        for k in range(variables):
            out_ref[k, r, into, :] = out_ref[k, r, into, :] + (0.5 * timestep) * total[k]

    def each_row(low, high, step):
        lax.fori_loop(low, high, lambda r, _: (step(r), 0)[1], 0)

    def each_edge(step):
        lax.fori_loop(
            0, 4, lambda i, _: (step(i + (i // 2) * (rows - 4)), 0)[1], 0
        )

    def all_tiles(step):
        def run(r):
            for t in range(tiles):
                step(r, t)

        return run

    for side, copy in enumerate(first_phi):
        copy.wait_recv()
        phi_unpack(first, 0, side, whole)
    each_row(2, rows - 2, all_tiles(section_one))
    each_edge(all_tiles(rest_one))
    radial_land(first_radial[0], first, 0)
    each_edge(lambda r: radial_one(r, 0))

    for copy in slab_copies:
        copy.wait_recv()
    before = jnp.zeros((1, lanes), jnp.float32)
    for j in range(slabs - 1, 0, -1):
        before = before + jnp.where(slab >= j, got[j * wedges], 0.0)
    before = jnp.sum(before, axis=1, keepdims=True)
    weight = jnp.where(lane < line, 1.0, jnp.where(lane == line, 0.5, 0.0))
    within = jnp.sum(weight * slab_part[...], axis=1, keepdims=True)
    enclosed = core[0] + before + within + jnp.zeros((rows, lanes), jnp.float32)
    mass_ref[...] = jnp.sum(jnp.where(lane == line, enclosed, 0.0), axis=0, keepdims=True)[:, :rows]
    pull[...] = strength * enclosed / (centres * centres)
    for t in range(tiles):
        if t:
            radial_land(first_radial[t], first, t)
            each_edge(lambda r: radial_one(r, t))
        each_edge(lambda r: late_gravity(r, t))
        radial_start(second_radial[t])
        for side, last in ((0, 0), (1, tiles - 1)):
            if t == last:
                phi_pack(second, 1, side, low_edge)
                phi_pack(second, 1, side, high_edge)
                low_phi[side].start()
                high_phi[side].start()
        if t == 0:
            each_row(2, rows - 2, all_tiles(late_gravity))
            for side, copy in enumerate(inside_phi):
                phi_pack(second, 1, side, inside)
                copy.start()
            for side, copy in enumerate(inside_phi):
                copy.wait_recv()
                phi_unpack(second, 1, side, inside)
        each_row(2, rows - 2, lambda r: section_two(r, t))
    for side in range(2):
        low_phi[side].wait_recv()
        high_phi[side].wait_recv()
        phi_unpack(second, 1, side, low_edge)
        phi_unpack(second, 1, side, high_edge)
    each_edge(all_tiles(lambda r, t: section_two(r, t, False)))
    for t in range(tiles):
        radial_land(second_radial[t], second, t)
        each_edge(lambda r: radial_two(r, t))

    for copy in part_copies + slab_copies + first_phi + inside_phi + low_phi + high_phi:
        copy.wait_send()
    for copies in first_radial + second_radial:
        radial_sent(copies)


def body(conserved, core_mass):
    variables, rows, cells, lanes = conserved.shape
    slabs, wedges = lax.axis_size("radial"), lax.axis_size("phi")
    sizes = step_sizes(rows * slabs, cells * wedges, lanes)
    table = jnp.asarray(angle_tables(lanes, sizes[1]))
    tiles = cells // TILE
    padded = (variables, rows + 4, cells + 2 * PAD, lanes)
    vmem = pl.BlockSpec(memory_space=pltpu.VMEM)
    dma = pltpu.SemaphoreType.DMA
    advanced, mass = pl.pallas_call(
        functools.partial(kernel, sizes, (slabs, wedges)),
        out_shape=(
            pltpu.VMEM(conserved.shape, jnp.float32),
            pltpu.VMEM((1, rows), jnp.float32),
        ),
        in_specs=[pl.BlockSpec(memory_space=pl.ANY)] * 3,
        out_specs=(vmem, vmem),
        scratch_shapes=[
            pltpu.VMEM(padded, jnp.float32),
            pltpu.VMEM(padded, jnp.float32),
            pltpu.VMEM((4, variables, rows, 2, lanes), jnp.float32),
            pltpu.VMEM((4, variables, rows, 2, lanes), jnp.float32),
            pltpu.VMEM((1, lanes), jnp.float32),
            pltpu.VMEM((1, lanes), jnp.float32),
            pltpu.VMEM((slabs * wedges, 1, lanes), jnp.float32),
            pltpu.VMEM((rows, lanes), jnp.float32),
            pltpu.VMEM((TILE, lanes), jnp.float32),
            pltpu.SMEM((1,), jnp.float32),
            dma((3,)),
            dma((4 * tiles,)),
            dma((4 * tiles,)),
            dma((8,)),
            dma((8,)),
            dma((slabs * wedges,)),
            dma((slabs * wedges,)),
        ],
        compiler_params=pltpu.CompilerParams(collective_id=0, has_side_effects=True),
    )(core_mass, table, conserved)
    return advanced, mass.reshape(rows)


def solution(mesh):
    in_specs = (P(None, "radial", "phi", None), P())
    out_specs = (P(None, "radial", "phi", None), P("radial"))
    return jax.shard_map(body, mesh=mesh, in_specs=in_specs, out_specs=out_specs, check_vma=False)
```

```python
import functools
import math

import jax
import jax.numpy as jnp
import numpy as np
from jax import lax
from jax.experimental import pallas as pl
from jax.experimental.pallas import tpu as pltpu
from jax.sharding import PartitionSpec as P

ADIABATIC = 4.0 / 3.0
INNER_RADIUS = 1.0
OUTER_RADIUS = 2.0
COURANT = 0.4
GRAVITY_KICK = 0.004
MINIMUM_DENSITY = 0.05
PRESSURE_FLOOR = 0.01
MESH = pl.DeviceIdType.MESH
TILE = 8
PAD = 8


def step_sizes(radial_total, phi_total, theta_total):
    theta_step = math.pi / theta_total
    phi_step = 2.0 * math.pi / phi_total
    polar_width = INNER_RADIUS * math.sin(0.5 * theta_step) * phi_step
    radial_step = min(2.0 * polar_width, (OUTER_RADIUS - INNER_RADIUS) / radial_total)
    timestep = COURANT * min(radial_step, polar_width)
    return (radial_step, theta_step, phi_step, timestep)


def angle_tables(theta_cells, theta_step):
    step = np.float32(theta_step)
    centre = (np.arange(theta_cells, dtype=np.float32) + np.float32(0.5)) * step
    face = np.arange(theta_cells + 1, dtype=np.float32) * step
    sine = np.sin(centre.astype(np.float64))
    cosine = np.cos(centre.astype(np.float64))
    face_sine = np.sin(face.astype(np.float64))
    zero = np.zeros(theta_cells)
    rows = [sine, face_sine[:-1], face_sine[1:], cosine / sine, 1.0 / sine, zero, zero, zero]
    return np.stack(rows).astype(np.float32)


def half_slope(below, above):
    return 0.5 * (
        jnp.maximum(jnp.minimum(below, above), 0.0) + jnp.minimum(jnp.maximum(below, above), 0.0)
    )


def thermo(q):
    density = jnp.maximum(q[0], MINIMUM_DENSITY)
    inverse = 1.0 / density
    kinetic = 0.5 * (q[1] * q[1] + q[2] * q[2] + q[3] * q[3]) * inverse
    pressure = jnp.maximum((ADIABATIC - 1.0) * (q[4] - kinetic), PRESSURE_FLOOR * density)
    return density, inverse, pressure


def physical(q, component):
    _, inverse, pressure = thermo(q)
    normal = q[component] * inverse
    squared = ADIABATIC * pressure * inverse
    return normal, pressure, jnp.abs(normal) + squared * lax.rsqrt(squared)


def flux(left, right, component):
    left_v, left_p, left_a = physical(left, component)
    right_v, right_p, right_a = physical(right, component)
    signal = jnp.maximum(left_a, right_a)
    left_w = 0.5 * (left_v + signal)
    right_w = 0.5 * (right_v - signal)
    out = [a * left_w + b * right_w for a, b in zip(left, right)]
    out[component] = out[component] + 0.5 * (left_p + right_p)
    out[4] = out[4] + 0.5 * (left_p * left_v + right_p * right_v)
    return out


def two_faces(rows, component):
    lower_left, lower_right, upper_left, upper_right = [], [], [], []
    for a, b, c, d, e in zip(*rows):
        ab, bc, cd, de = b - a, c - b, d - c, e - d
        sb, sc, sd = half_slope(ab, bc), half_slope(bc, cd), half_slope(cd, de)
        lower_left.append(b + sb)
        lower_right.append(c - sc)
        upper_left.append(c + sc)
        upper_right.append(d - sd)
    return flux(lower_left, lower_right, component), flux(upper_left, upper_right, component)


def kernel(
    sizes,
    counts,
    core_ref,
    table_ref,
    input_ref,
    out_ref,
    mass_ref,
    first,
    second,
    edge,
    halo,
    part,
    slab_part,
    got,
    pull,
    table,
    core,
    load_sem,
    radial_send,
    radial_recv,
    phi_send,
    phi_recv,
    part_send,
    part_recv,
):
    radial_step, theta_step, phi_step, timestep = sizes
    slabs, wedges = counts
    variables, rows, cells, lanes = input_ref.shape
    tiles = cells // TILE
    strength = GRAVITY_KICK / timestep
    slab, wedge = lax.axis_index("radial"), lax.axis_index("phi")
    has_up, has_down = slab < slabs - 1, slab > 0

    load = pltpu.make_async_copy(
        input_ref, first.at[:, pl.ds(2, rows), pl.ds(PAD, cells), :], load_sem.at[0]
    )
    load.start()
    load_table = pltpu.make_async_copy(table_ref, table, load_sem.at[1])
    load_table.start()
    load_core = pltpu.make_async_copy(core_ref, core, load_sem.at[2])
    load_core.start()

    def radial_peer(jump):
        return (lax.rem(slab + jump, slabs), wedge)

    def phi_peer(jump):
        return (slab, lax.rem(wedge + jump, wedges))

    barrier = pltpu.get_barrier_semaphore()
    jumps = [(i, 0) for i in range(1, slabs)] + [(0, j) for j in range(1, wedges)]

    def peer_at(jump):
        return (radial_peer(jump[0])[0], phi_peer(jump[1])[1])

    for jump in jumps:
        pl.semaphore_signal(barrier, inc=1, device_id=peer_at(jump), device_id_type=MESH)
    load.wait()
    load_table.wait()
    load_core.wait()

    def remote(src, dst, send, recv, peer):
        return pltpu.make_async_remote_copy(
            src_ref=src, dst_ref=dst, send_sem=send, recv_sem=recv, device_id=peer,
            device_id_type=MESH,
        )

    def radial_copies(buffer, section, tile):
        where = pl.ds(PAD + TILE * tile, TILE)
        slot = (section * tiles + tile) * 2
        up = remote(
            buffer.at[:, pl.ds(rows, 2), where, :], buffer.at[:, pl.ds(0, 2), where, :],
            radial_send.at[slot], radial_recv.at[slot], radial_peer(1),
        )
        down = remote(
            buffer.at[:, pl.ds(2, 2), where, :], buffer.at[:, pl.ds(rows + 2, 2), where, :],
            radial_send.at[slot + 1], radial_recv.at[slot + 1], radial_peer(slabs - 1),
        )
        return up, down

    def radial_start(copies):
        up, down = copies

        @pl.when(has_up)
        def _():
            up.start()

        @pl.when(has_down)
        def _():
            down.start()

    def radial_sent(copies):
        up, down = copies

        @pl.when(has_up)
        def _():
            up.wait_send()

        @pl.when(has_down)
        def _():
            down.wait_send()

    def radial_land(copies, buffer, tile):
        up, down = copies
        where = pl.ds(PAD + TILE * tile, TILE)

        @pl.when(has_down)
        def _():
            up.wait_recv()

        @pl.when(jnp.logical_not(has_down))
        def _():
            value = buffer[:, 2, where, :]
            buffer[:, 0, where, :] = value
            buffer[:, 1, where, :] = value

        @pl.when(has_up)
        def _():
            down.wait_recv()

        @pl.when(jnp.logical_not(has_up))
        def _():
            value = buffer[:, rows + 1, where, :]
            buffer[:, rows + 2, where, :] = value
            buffer[:, rows + 3, where, :] = value

    whole, inside, low_edge, high_edge = (0, rows), (2, rows - 4), (0, 2), (rows - 2, 2)

    def phi_copies(section, piece, slot):
        where = pl.ds(*piece)
        return [
            remote(
                edge.at[section * 2 + side, :, where], halo.at[section * 2 + side, :, where],
                phi_send.at[slot + side], phi_recv.at[slot + side], phi_peer(jump),
            )
            for side, jump in ((0, wedges - 1), (1, 1))
        ]

    def phi_pack(buffer, section, side, piece):
        begin, count = piece
        start = PAD if side == 0 else PAD + cells - 2
        edge[section * 2 + side, :, pl.ds(begin, count)] = buffer[
            :, pl.ds(2 + begin, count), pl.ds(start, 2), :
        ]

    def phi_unpack(buffer, section, side, piece):
        begin, count = piece
        start = PAD + cells if side == 0 else PAD - 2
        buffer[:, pl.ds(2 + begin, count), pl.ds(start, 2), :] = halo[
            section * 2 + side, :, pl.ds(begin, count)
        ]

    shape = (TILE, lanes)
    lane = lax.broadcasted_iota(jnp.int32, (rows, lanes), 1)
    line = lax.broadcasted_iota(jnp.int32, (rows, lanes), 0)
    column = jnp.sum(first[0, pl.ds(2, rows), pl.ds(PAD, cells), :], axis=1)
    column = jnp.sum(column * table[0:1, :], axis=1, keepdims=True)
    centres = INNER_RADIUS + (
        (slab * rows + line).astype(jnp.float32) + 0.5
    ) * radial_step
    column = column * centres * centres * (radial_step * theta_step * phi_step)
    part[...] = jnp.sum(jnp.where(lane == line, column, 0.0), axis=0, keepdims=True)
    got[0] = part[...]
    phi_pack(first, 0, 0, whole)
    phi_pack(first, 0, 1, whole)
    pl.semaphore_wait(barrier, len(jumps))

    def wedge_sum():
        shells = jnp.zeros((1, lanes), jnp.float32)
        for w in range(wedges):
            shells = shells + got[lax.rem(wedge + wedges - w, wedges)]
        return shells

    part_copies = []
    for j in range(1, wedges):
        i, slot = 0, j
        part_copies.append(
            remote(part, got.at[slot], part_send.at[slot], part_recv.at[slot], peer_at((i, j)))
        )
    first_radial = [radial_copies(first, 0, t) for t in range(tiles)]
    second_radial = [radial_copies(second, 1, t) for t in range(tiles)]
    first_phi = phi_copies(0, whole, 0)
    inside_phi = phi_copies(1, inside, 2)
    low_phi, high_phi = phi_copies(1, low_edge, 4), phi_copies(1, high_edge, 6)
    for copy in part_copies + first_phi:
        copy.start()
    radial_start(first_radial[0])
    for copy in part_copies:
        copy.wait_recv()
    slab_part[...] = wedge_sum()
    slab_copies = []
    for j in range(1, slabs):
        slot = j * wedges
        slab_copies.append(
            remote(
                slab_part, got.at[slot], part_send.at[slot], part_recv.at[slot], radial_peer(j)
            )
        )
    for copy in slab_copies:
        copy.start()
    for t in range(1, tiles):
        radial_start(first_radial[t])

    lane_tile = lax.broadcasted_iota(jnp.int32, shape, 1)
    is_first, is_last = lane_tile == 0, lane_tile == lanes - 1

    def rate(buffer, r, tile, radial=True, rest=True):
        start = PAD + TILE * tile

        def at(row, offset):
            return [buffer[k, row + 2, pl.ds(start + offset, TILE), :] for k in range(variables)]

        def spread(value):
            return jnp.broadcast_to(value, shape)

        index = jnp.full(shape, slab * rows + r, jnp.int32).astype(jnp.float32)
        radius = INNER_RADIUS + (index + 0.5) * radial_step
        inner, outer = radius - 0.5 * radial_step, radius + 0.5 * radial_step
        inverse_r = 1.0 / radius
        centre = at(r, 0)
        total = [0.0] * variables
        if radial:
            lower, upper = two_faces([at(r + o, 0) if o else centre for o in range(-2, 3)], 1)
            scale = inverse_r * inverse_r * (1.0 / radial_step)
            area_in, area_out = inner * inner * scale, outer * outer * scale
            total = [area_in * a - area_out * b for a, b in zip(lower, upper)]
        if not rest:
            return total
        lower, upper = two_faces([at(r, o) if o else centre for o in range(-2, 3)], 3)
        around = inverse_r * spread(table[4:5, :])
        scale = around * (1.0 / phi_step)
        total = [t + (a - b) * scale for t, a, b in zip(total, lower, upper)]
        left, right = [], []
        for q in centre:
            after = jnp.where(is_last, q, pltpu.roll(q, lanes - 1, 1))
            above = after - q
            below = jnp.where(is_first, 0.0, pltpu.roll(above, 1, 1))
            slope = half_slope(below, above)
            left.append(q + slope)
            right.append(jnp.where(is_last, q, pltpu.roll(q - slope, lanes - 1, 1)))
        upper = flux(left, right, 2)
        scale = around * (1.0 / theta_step)
        low_sine, high_sine = spread(table[1:2, :]), spread(table[2:3, :])
        low_area, high_area = low_sine * scale, high_sine * scale
        total = [
            t + (low_area * pltpu.roll(f, 1, 1) - high_area * f) for t, f in zip(total, upper)
        ]
        density, inverse, pressure = thermo(centre)
        vr, vt, vp = (centre[m] * inverse for m in (1, 2, 3))
        cot = spread(table[3:4, :])
        total[1] = total[1] + (2.0 * pressure + density * (vt * vt + vp * vp)) * inverse_r
        total[2] = total[2] + (
            (pressure + density * vp * vp) * cot - density * vr * vt
        ) * inverse_r
        total[3] = total[3] - density * vp * (vr + vt * cot) * inverse_r
        return centre, density, total

    def gravity_at(r):
        return jnp.broadcast_to(pull[pl.ds(r, 1), :], shape)

    def with_gravity(rates, r):
        centre, density, total = rates
        gravity = gravity_at(r)
        total[1] = total[1] - density * gravity
        total[4] = total[4] - centre[1] * gravity
        return centre, total

    def section_one(r, tile):
        centre, _, total = rate(first, r, tile)
        where = pl.ds(PAD + TILE * tile, TILE)
        for k in range(variables):
            second[k, r + 2, where, :] = centre[k] + timestep * total[k]

    def rest_one(r, tile):
        centre, _, total = rate(first, r, tile, radial=False)
        where = pl.ds(PAD + TILE * tile, TILE)
        for k in range(variables):
            second[k, r + 2, where, :] = centre[k] + timestep * total[k]

    def radial_one(r, tile):
        total = rate(first, r, tile, rest=False)
        where = pl.ds(PAD + TILE * tile, TILE)
        for k in range(variables):
            second[k, r + 2, where, :] = second[k, r + 2, where, :] + timestep * total[k]

    def late_gravity(r, tile):
        where = pl.ds(PAD + TILE * tile, TILE)
        gravity = timestep * gravity_at(r)
        density = jnp.maximum(first[0, r + 2, where, :], MINIMUM_DENSITY)
        second[1, r + 2, where, :] = second[1, r + 2, where, :] - density * gravity
        second[4, r + 2, where, :] = (
            second[4, r + 2, where, :] - first[1, r + 2, where, :] * gravity
        )

    def section_two(r, tile, radial=True):
        centre, total = with_gravity(rate(second, r, tile, radial=radial), r)
        where = pl.ds(PAD + TILE * tile, TILE)
        into = pl.ds(TILE * tile, TILE)
        for k in range(variables):
            begin = first[k, r + 2, where, :]
            out_ref[k, r, into, :] = 0.5 * begin + 0.5 * (centre[k] + timestep * total[k])

    def radial_two(r, tile):
        total = rate(second, r, tile, rest=False)
        into = pl.ds(TILE * tile, TILE)
        for k in range(variables):
            out_ref[k, r, into, :] = out_ref[k, r, into, :] + (0.5 * timestep) * total[k]

    def each_row(low, high, step):
        lax.fori_loop(low, high, lambda r, _: (step(r), 0)[1], 0)

    def each_edge(step):
        lax.fori_loop(
            0, 4, lambda i, _: (step(i + (i // 2) * (rows - 4)), 0)[1], 0
        )

    def all_tiles(step):
        def run(r):
            for t in range(tiles):
                step(r, t)

        return run

    for side, copy in enumerate(first_phi):
        copy.wait_recv()
        phi_unpack(first, 0, side, whole)
    each_row(2, rows - 2, all_tiles(section_one))
    each_edge(all_tiles(rest_one))
    radial_land(first_radial[0], first, 0)
    each_edge(lambda r: radial_one(r, 0))

    for copy in slab_copies:
        copy.wait_recv()
    before = jnp.zeros((1, lanes), jnp.float32)
    for j in range(slabs - 1, 0, -1):
        before = before + jnp.where(slab >= j, got[j * wedges], 0.0)
    before = jnp.sum(before, axis=1, keepdims=True)
    weight = jnp.where(lane < line, 1.0, jnp.where(lane == line, 0.5, 0.0))
    within = jnp.sum(weight * slab_part[...], axis=1, keepdims=True)
    enclosed = core[0] + before + within + jnp.zeros((rows, lanes), jnp.float32)
    mass_ref[...] = jnp.sum(jnp.where(lane == line, enclosed, 0.0), axis=0, keepdims=True)[:, :rows]
    pull[...] = strength * enclosed / (centres * centres)
    for t in range(tiles):
        if t:
            radial_land(first_radial[t], first, t)
            each_edge(lambda r: radial_one(r, t))
        each_edge(lambda r: late_gravity(r, t))
        radial_start(second_radial[t])
        for side, last in ((0, 0), (1, tiles - 1)):
            if t == last:
                phi_pack(second, 1, side, low_edge)
                phi_pack(second, 1, side, high_edge)
                low_phi[side].start()
                high_phi[side].start()
        if t == 0:
            each_row(2, rows - 2, all_tiles(late_gravity))
            for side, copy in enumerate(inside_phi):
                phi_pack(second, 1, side, inside)
                copy.start()
    for side, copy in enumerate(inside_phi):
        copy.wait_recv()
        phi_unpack(second, 1, side, inside)
    each_row(2, rows - 2, all_tiles(section_two))
    for side in range(2):
        low_phi[side].wait_recv()
        high_phi[side].wait_recv()
        phi_unpack(second, 1, side, low_edge)
        phi_unpack(second, 1, side, high_edge)
    each_edge(all_tiles(lambda r, t: section_two(r, t, False)))
    for t in range(tiles):
        radial_land(second_radial[t], second, t)
        each_edge(lambda r: radial_two(r, t))

    for copy in part_copies + slab_copies + first_phi + inside_phi + low_phi + high_phi:
        copy.wait_send()
    for copies in first_radial + second_radial:
        radial_sent(copies)


def body(conserved, core_mass):
    variables, rows, cells, lanes = conserved.shape
    slabs, wedges = lax.axis_size("radial"), lax.axis_size("phi")
    sizes = step_sizes(rows * slabs, cells * wedges, lanes)
    table = jnp.asarray(angle_tables(lanes, sizes[1]))
    tiles = cells // TILE
    padded = (variables, rows + 4, cells + 2 * PAD, lanes)
    vmem = pl.BlockSpec(memory_space=pltpu.VMEM)
    dma = pltpu.SemaphoreType.DMA
    advanced, mass = pl.pallas_call(
        functools.partial(kernel, sizes, (slabs, wedges)),
        out_shape=(
            pltpu.VMEM(conserved.shape, jnp.float32),
            pltpu.VMEM((1, rows), jnp.float32),
        ),
        in_specs=[pl.BlockSpec(memory_space=pl.ANY)] * 3,
        out_specs=(vmem, vmem),
        scratch_shapes=[
            pltpu.VMEM(padded, jnp.float32),
            pltpu.VMEM(padded, jnp.float32),
            pltpu.VMEM((4, variables, rows, 2, lanes), jnp.float32),
            pltpu.VMEM((4, variables, rows, 2, lanes), jnp.float32),
            pltpu.VMEM((1, lanes), jnp.float32),
            pltpu.VMEM((1, lanes), jnp.float32),
            pltpu.VMEM((slabs * wedges, 1, lanes), jnp.float32),
            pltpu.VMEM((rows, lanes), jnp.float32),
            pltpu.VMEM((TILE, lanes), jnp.float32),
            pltpu.SMEM((1,), jnp.float32),
            dma((3,)),
            dma((4 * tiles,)),
            dma((4 * tiles,)),
            dma((8,)),
            dma((8,)),
            dma((slabs * wedges,)),
            dma((slabs * wedges,)),
        ],
        compiler_params=pltpu.CompilerParams(collective_id=0, has_side_effects=True),
    )(core_mass, table, conserved)
    return advanced, mass.reshape(rows)


def solution(mesh):
    in_specs = (P(None, "radial", "phi", None), P())
    out_specs = (P(None, "radial", "phi", None), P("radial"))
    return jax.shard_map(body, mesh=mesh, in_specs=in_specs, out_specs=out_specs, check_vma=False)
```
